16 devices in a mesh: dp: 2 (over y, z), tp: 8 (over x, core).
Axes of the slice: x: 4, y: 2, z: 1, core: 2. Of those that a mesh axis runs over, the one named last changes fastest.
The devices are a block of a 4x4x8 slice.
Arguments:
- hidden: bfloat16 [4, 2048, 512], P('dp', 'tp'), parts along dimension 0
- grad_out: bfloat16 [4, 2048, 512], P('dp', 'tp'), parts along dimension 0
- ln1_gain: bfloat16 [512], replicated
- ln1_bias: bfloat16 [512], replicated
- w_qkv: bfloat16 [512, 3, 8, 64], P(None, None, 'tp')
- b_qkv: bfloat16 [3, 8, 64], P(None, 'tp')
- w_out: bfloat16 [8, 64, 512], P('tp')
- b_out: bfloat16 [512], replicated
- ln2_gain: bfloat16 [512], replicated
- ln2_bias: bfloat16 [512], replicated
- w_up: bfloat16 [512, 2048], P(None, 'tp')
- b_up: bfloat16 [2048], P('tp')
- w_down: bfloat16 [2048, 512], P('tp')
- b_down: bfloat16 [512], replicated
Outputs:
- output 1: bfloat16 [4, 2048, 512], P('dp', 'tp'), parts along dimension 0
- output 2: bfloat16 [4, 2048, 512], P('dp', 'tp'), parts along dimension 0
- output 3: float32 [1024], P('dp'), parts along dimension 0
- output 4: float32 [1024], P('dp'), parts along dimension 0
- output 5: float32 [1024, 3, 8, 64], P('dp', None, 'tp'), parts along dimension 0
- output 6: float32 [6, 8, 64], P('dp', 'tp'), parts along dimension 0
- output 7: float32 [16, 64, 512], P(('dp', 'tp')), parts along dimension 0
- output 8: float32 [1024], P('dp'), parts along dimension 0
- output 9: float32 [1024], P('dp'), parts along dimension 0
- output 10: float32 [1024], P('dp'), parts along dimension 0
- output 11: float32 [1024, 2048], P('dp', 'tp'), parts along dimension 0
- output 12: float32 [4096], P(('dp', 'tp')), parts along dimension 0
- output 13: float32 [4096, 512], P(('dp', 'tp')), parts along dimension 0
- output 14: float32 [1024], P('dp'), parts along dimension 0
There are 2 independent parts. The reference program is written for one: setup_inputs(seed, part) draws one part's arguments, and reference() takes and returns one part's arrays. A program takes and returns all parts, laid end to end along the dimension named above; an argument that names none is the same for every part.
All inputs are finite; a program needn't handle non-finite values.
Results may differ from the reference program's by a relative error of at most 0.0187336.
Values are sent between devices in bfloat16 or wider.
A program may use at most 768 MiB of HBM per device.

```python
import jax
import jax.numpy as jnp
from jax import lax

D_MODEL = 512
HEADS = 8
HEAD_DIM = 64
FF_DIM = 2048
BATCH = 2
SEQ_LEN = 2048
LN_EPS = 1e-5


def draw_normal(key, shape, scale):
    return jax.random.normal(key, shape, jnp.float32) * scale


def setup_inputs(seed: int = 0, part: int = 0) -> dict:
    base_key = jax.random.key(seed)
    act_keys = jax.random.split(jax.random.fold_in(base_key, part), 2)
    weight_keys = jax.random.split(jax.random.fold_in(base_key, 100003), 12)
    d_scale = D_MODEL ** -0.5
    inputs = {
        "hidden": draw_normal(act_keys[0], (BATCH, SEQ_LEN, D_MODEL), 1.0),
        "grad_out": draw_normal(act_keys[1], (BATCH, SEQ_LEN, D_MODEL), 1.0),
        "ln1_gain": 1.0 + draw_normal(weight_keys[0], (D_MODEL,), 0.3),
        "ln1_bias": draw_normal(weight_keys[1], (D_MODEL,), 0.3),
        "w_qkv": draw_normal(weight_keys[2], (D_MODEL, 3, HEADS, HEAD_DIM), d_scale),
        "b_qkv": draw_normal(weight_keys[3], (3, HEADS, HEAD_DIM), 0.5),
        "w_out": draw_normal(weight_keys[4], (HEADS, HEAD_DIM, D_MODEL), d_scale),
        "b_out": draw_normal(weight_keys[5], (D_MODEL,), 0.3),
        "ln2_gain": 1.0 + draw_normal(weight_keys[6], (D_MODEL,), 0.3),
        "ln2_bias": draw_normal(weight_keys[7], (D_MODEL,), 0.3),
        "w_up": draw_normal(weight_keys[8], (D_MODEL, FF_DIM), d_scale),
        "b_up": draw_normal(weight_keys[9], (FF_DIM,), 0.3),
        "w_down": draw_normal(weight_keys[10], (FF_DIM, D_MODEL), FF_DIM ** -0.5),
        "b_down": draw_normal(weight_keys[11], (D_MODEL,), 0.3),
    }
    return {name: value.astype(jnp.bfloat16) for name, value in inputs.items()}


def as_bf16(value):
    return value.astype(jnp.bfloat16).astype(jnp.float32)


def layer_norm(value, gain, shift):
    centered = value - jnp.mean(value, axis=-1, keepdims=True)
    variance = jnp.mean(centered * centered, axis=-1, keepdims=True)
    return centered * lax.rsqrt(variance + LN_EPS) * gain + shift


def layer_forward(params, hidden):
    ln1_gain, ln1_bias, w_qkv, b_qkv, w_out, b_out, ln2_gain, ln2_bias, w_up, b_up, w_down, b_down = params
    normed1 = as_bf16(layer_norm(hidden, ln1_gain, ln1_bias))
    qkv_proj = as_bf16(jnp.einsum("bsd,dche->bsche", normed1, w_qkv) + b_qkv)
    scores = jnp.einsum("bqhe,bkhe->bhqk", qkv_proj[:, :, 0], qkv_proj[:, :, 1]) * (HEAD_DIM ** -0.5)
    positions = jnp.arange(SEQ_LEN)
    causal = positions[:, None] >= positions[None, :]
    attn_probs = as_bf16(jax.nn.softmax(jnp.where(causal, scores, -1e30), axis=-1))
    context = as_bf16(jnp.einsum("bhqk,bkhe->bqhe", attn_probs, qkv_proj[:, :, 2]))
    resid1 = as_bf16(hidden + jnp.einsum("bqhe,hed->bqd", context, w_out) + b_out)
    normed2 = as_bf16(layer_norm(resid1, ln2_gain, ln2_bias))
    pre_act = as_bf16(jnp.einsum("bsd,df->bsf", normed2, w_up) + b_up)
    gelu_out = as_bf16(jax.nn.gelu(pre_act, approximate=True))
    return as_bf16(resid1 + jnp.einsum("bsf,fd->bsd", gelu_out, w_down) + b_down)


def reference(hidden, grad_out, ln1_gain, ln1_bias, w_qkv, b_qkv, w_out, b_out, ln2_gain, ln2_bias, w_up, b_up, w_down, b_down):
    weights = (ln1_gain, ln1_bias, w_qkv, b_qkv, w_out, b_out, ln2_gain, ln2_bias, w_up, b_up, w_down, b_down)
    params = tuple(param.astype(jnp.float32) for param in weights)
    layer_out, pullback = jax.vjp(layer_forward, params, hidden.astype(jnp.float32))
    grad_params, grad_hidden = pullback(grad_out.astype(jnp.float32))
    return (layer_out.astype(jnp.bfloat16), grad_hidden.astype(jnp.bfloat16), grad_params[0], grad_params[1], grad_params[2], grad_params[3], grad_params[4], grad_params[5], grad_params[6], grad_params[7], grad_params[8], grad_params[9], grad_params[10], grad_params[11])
```

```python
import jax
import jax.numpy as jnp
from jax import lax
from jax.experimental import pallas as pl
from jax.experimental.pallas import tpu as pltpu
from jax.sharding import PartitionSpec as P

LN_EPS = 1e-5
MESH = pl.DeviceIdType.MESH
F32 = jnp.float32
BF16 = jnp.bfloat16
LOG2E = 1.4426950408889634
GELU_A = 0.7978845608028654
GELU_B = 0.044715

W2_ROW, W1_ROW, WO_ROW, WQ_ROW, BU_ROW, W_ROWS, W_CUT = 0, 256, 512, 576, 768, 784, 384
DB_ROW, G_ROWS, G_HALF = 576, 592, 296


def mm(lhs, rhs, lc=1, rc=0):
    return lax.dot_general(lhs, rhs, (((lc,), (rc,)), ((), ())), preferred_element_type=F32)


def norm_stats(value):
    centered = value - jnp.mean(value, axis=-1, keepdims=True)
    inv_std = lax.rsqrt(jnp.mean(centered * centered, axis=-1, keepdims=True) + LN_EPS)
    return centered * inv_std, inv_std


def norm_back(grad, x_hat, inv_std, gain):
    scaled = grad * gain
    return inv_std * (scaled - jnp.mean(scaled, axis=-1, keepdims=True) - x_hat * jnp.mean(scaled * x_hat, axis=-1, keepdims=True))


def layer_kernel(n_dev, attn_scale,
                 x, dy, g1, s1, bo, g2, s2, bd, wqkv, bqkv, wo, wu, bu, wd,
                 y_out, dx_out, vec_out, dwqkv_out, dbqkv_out, dwo_out, dwu_out, dbu_out, dwd_out,
                 h1, wp, q_s, k_s, v_s, qkvt, s_scr, lse, o_own, o_all, wo_all, x1, h2, ga, dza, acc, dx1, do_send, do_all, do_s,
                 delta, dqt, dk_s, dv_s, dqkvt, dqkvt_all, dwp, dwr, r_a, r_b, r_l, r_r, vec, vec_all,
                 ag_ss, ag_rs, o_ss, o_rs, do_ss, do_rs, dq_ss, dq_rs, dw_ss, dw_rs, v_ss, v_rs):
    me = lax.axis_index("tp")
    chips = n_dev // 2
    chip, core = lax.div(me, 2), lax.rem(me, 2)

    def dev(shift, other):
        return 2 * lax.rem(chip + shift + chips, chips) + (1 - core if other else core)

    L, R, O, PT = dev(-1, False), dev(1, False), dev(2, False), dev(0, True)
    PL, PR, PO = dev(-1, True), dev(1, True), dev(2, True)

    def rc(src, dst, ssem, rsem, target):
        return pltpu.make_async_remote_copy(src_ref=src, dst_ref=dst, send_sem=ssem, recv_sem=rsem,
                                            device_id={"tp": target}, device_id_type=MESH)

    def m256(i):
        return pl.ds(pl.multiple_of(i * 256, 256), 256)

    plan = ((me, "F", R, L), (me, "F", L, R), (me, "F", PT, PT), (L, "A", R, O), (R, "B", L, O),
            (L, "F", PT, PL), (R, "F", PT, PR), (O, "A", PT, PO), (O, "B", PT, PO))

    def view(a, owner, part):
        if a < 2:
            off, size = {"F": (0, 256), "A": (0, 128), "B": (128, 128)}[part]
            return h1.at[a, pl.ds(pl.multiple_of(owner * 256 + off, 128), size), :]
        off, size = {"F": (0, W_ROWS), "A": (0, W_CUT), "B": (W_CUT, W_ROWS - W_CUT)}[part]
        return wp.at[owner, pl.ds(off, size), :]

    def ag_copy(a, ch, received):
        own, part, target, got = plan[ch]
        v = view(a, got if received else own, part)
        return rc(v, v, ag_ss.at[a, ch], ag_rs.at[a, ch], target)

    def ag_start(a, *chs):
        for ch in chs:
            ag_copy(a, ch, False).start()

    def ag_wait(a, *chs):
        for ch in chs:
            ag_copy(a, ch, True).wait_recv()

    barrier = pltpu.get_barrier_semaphore()
    for i in range(n_dev):
        @pl.when(me != i)
        def _():
            pl.semaphore_signal(barrier, inc=1, device_id={"tp": i}, device_id_type=MESH)

    gain1, shift1 = g1[...].astype(F32), s1[...].astype(F32)
    for b in range(2):
        for r in range(2):
            rows = slice(b * 256 + r * 128, b * 256 + r * 128 + 128)
            x_hat, _ = norm_stats(x[rows, :].astype(F32))
            h1[b, pl.ds(pl.multiple_of(me * 256 + r * 128, 128), 128), :] = (x_hat * gain1 + shift1).astype(BF16)

    pl.semaphore_wait(barrier, n_dev - 1)
    for b in range(2):
        ag_start(b, 0, 1, 2)

    wp[me, W2_ROW:W1_ROW, :] = wd[...]
    wp[me, W1_ROW:WO_ROW, :] = wu[...].astype(F32).T.astype(BF16)
    wp[me, WO_ROW:WQ_ROW, :] = wo[...]
    wp[me, WQ_ROW:BU_ROW, :] = wqkv[...].astype(F32).T[:192, :].astype(BF16)
    wp[me, BU_ROW:W_ROWS, 0:256] = jnp.broadcast_to(bu[...].astype(F32), (16, 256)).astype(BF16)
    wp[me, BU_ROW:W_ROWS, 256:512] = jnp.zeros((16, 256), BF16)

    bias_qkv = bqkv[...].astype(F32)

    def project(b, owner):
        rows = m256(owner)
        full = (mm(h1[b, rows, :], wqkv[...]) + bias_qkv).astype(BF16).astype(F32)
        q_s[b, rows, :] = full[:, 0:64].astype(BF16)
        k_s[b, rows, :] = full[:, 64:128].astype(BF16)
        v_s[b, rows, :] = full[:, 128:192].astype(BF16)
        qkvt[b, :, rows] = full.T[:192, :].astype(BF16)

    for b in range(2):
        project(b, me)
    for b in range(2):
        ag_wait(b, 0)
        ag_start(b, 3, 5)
        ag_wait(b, 1)
        ag_start(b, 4, 6)
        ag_wait(b, 2)
        if b == 1:
            ag_start(2, 0, 1, 2)
        for owner in (PT, L, R):
            project(b, owner)

    s_fac = attn_scale * LOG2E

    def causal(shape):
        return lax.broadcasted_iota(jnp.int32, shape, 0) <= lax.broadcasted_iota(jnp.int32, shape, 1)

    def o_copy(b, j, src):
        lanes = pl.ds(b * 256, 256)
        return rc(o_own.at[b, :, m256(j)], o_all.at[pl.ds(pl.multiple_of(src * 64, 64), 64), lanes],
                  o_ss.at[b, j], o_rs.at[b, src], j)

    def attend(b, j):
        cols = m256(j)
        q_t = qkvt[b, 0:64, cols]

        def scores(kc, m):
            s = mm(k_s[b, m256(kc), :], q_t) * s_fac
            s_scr[m256(kc), :] = s
            return jnp.maximum(m, jnp.max(s, axis=0, keepdims=True))

        s_d = jnp.where(causal((256, 256)), mm(k_s[b, cols, :], q_t) * s_fac, -1e30)
        s_scr[cols, :] = s_d
        m = lax.fori_loop(0, j, scores, jnp.max(s_d, axis=0, keepdims=True))

        def sums(kc, l):
            return l + jnp.sum(jnp.exp2(s_scr[m256(kc), :] - m), axis=0, keepdims=True)

        l = lax.fori_loop(0, j + 1, sums, jnp.zeros((1, 256), F32))
        lse_j = m + jnp.log2(l)
        lse[b, :, cols] = lse_j

        def outs(kc, o):
            p = jnp.exp2(s_scr[m256(kc), :] - lse_j).astype(BF16)
            return o + mm(qkvt[b, 128:192, m256(kc)], p)

        o = lax.fori_loop(0, j + 1, outs, jnp.zeros((64, 256), F32)).astype(BF16)
        o_own[b, :, cols] = o

        @pl.when(j != me)
        def _():
            o_copy(b, j, me).start()

        @pl.when(j == me)
        def _():
            o_all[pl.ds(pl.multiple_of(me * 64, 64), 64), pl.ds(b * 256, 256)] = o

    for b in range(2):
        ag_wait(b, 3)
        ag_start(b, 7)
        ag_wait(b, 4)
        ag_start(b, 8)
        project(b, O)
        ag_wait(b, 5, 6)
        project(b, PL)
        project(b, PR)
        ag_wait(b, 7, 8)
        project(b, PO)

        @pl.loop(0, n_dev)
        def _(j):
            attend(b, j)

    ag_wait(2, 0)
    ag_start(2, 3, 5)
    ag_wait(2, 1)
    ag_start(2, 4, 6)
    ag_wait(2, 2, 5, 6, 3)
    ag_start(2, 7)
    ag_wait(2, 4)
    ag_start(2, 8)
    ag_wait(2, 7, 8)
    for n in range(n_dev):
        wo_all[n * 64:(n + 1) * 64, :] = wp[n, WO_ROW:WQ_ROW, :]
    for b in range(2):
        for src in range(n_dev):
            @pl.when(me != src)
            def _():
                o_copy(b, me, src).wait_recv()

    bias_o = bo[...].astype(F32)
    gain2, shift2 = g2[...].astype(F32), s2[...].astype(F32)
    for r in range(4):
        rows = slice(r * 128, r * 128 + 128)
        attn = mm(o_all[:, rows], wo_all[...], 0, 0)
        x1_r = (x[rows, :].astype(F32) + attn + bias_o).astype(BF16)
        x1[rows, :] = x1_r
        x_hat, _ = norm_stats(x1_r.astype(F32))
        h2[rows, :] = (x_hat * gain2 + shift2).astype(BF16)
    acc[...] = jnp.zeros_like(acc)

    @pl.loop(0, n_dev)
    def _(n):
        w1t = wp[n, W1_ROW:WO_ROW, :]
        w2 = wp[n, W2_ROW:W1_ROW, :]
        bias_u = wp[n, BU_ROW:W_ROWS, 0:256].astype(F32)[0:1, :]
        for r in range(2):
            rows = slice(r * 256, r * 256 + 256)
            z = (mm(h2[rows, :], w1t, 1, 1) + bias_u).astype(BF16).astype(F32)
            z2 = z * z
            t = jnp.tanh(GELU_A * (z + GELU_B * z2 * z))
            ga[n, rows, :] = (0.5 * z * (1.0 + t)).astype(BF16)
            slope = 0.5 * (1.0 + t) + 0.5 * z * (1.0 - t * t) * (GELU_A * (1.0 + 3.0 * GELU_B * z2))
            dgl = mm(dy[rows, :], w2, 1, 1).astype(BF16).astype(F32)
            dz = (dgl * slope).astype(BF16)
            dza[n, rows, :] = dz
            acc[rows, :] += mm(dz, w1t)

    vec[...] = jnp.zeros_like(vec)
    for r in range(4):
        rows = slice(r * 128, r * 128 + 128)
        dh2 = acc[rows, :].astype(BF16).astype(F32)
        x_hat, inv_std = norm_stats(x1[rows, :].astype(F32))
        dy_r = dy[rows, :].astype(F32)
        dx1_r = (dy_r + norm_back(dh2, x_hat, inv_std, gain2)).astype(BF16)
        dx1[rows, :] = dx1_r
        vec[2:3, :] += jnp.sum(dx1_r.astype(F32), axis=0, keepdims=True)
        vec[3:4, :] += jnp.sum(dh2 * x_hat, axis=0, keepdims=True)
        vec[4:5, :] += jnp.sum(dh2, axis=0, keepdims=True)
        vec[5:6, :] += jnp.sum(dy_r, axis=0, keepdims=True)

    def do_copy(n, src):
        return rc(do_send.at[pl.ds(pl.multiple_of(n * 64, 64), 64), :], do_all.at[src], do_ss.at[n], do_rs.at[src], n)

    for r in range(2):
        rows = slice(r * 256, r * 256 + 256)
        do_send[rows, :] = mm(wo_all[rows, :], dx1[...], 1, 1).astype(BF16)
    for n in range(n_dev):
        @pl.when(me != n)
        def _():
            do_copy(n, me).start()
    do_all[me] = do_send[pl.ds(pl.multiple_of(me * 64, 64), 64), :]

    def grads(n):
        for r in range(2):
            cols = slice(r * 128, r * 128 + 128)
            dwp[n, W2_ROW + r * 128:W2_ROW + r * 128 + 128, :] = mm(ga[n, :, cols], dy[...], 0, 0)
            dwp[n, W1_ROW + r * 128:W1_ROW + r * 128 + 128, :] = mm(dza[n, :, cols], h2[...], 0, 0)
        dwp[n, WO_ROW:DB_ROW, :] = mm(o_all[pl.ds(pl.multiple_of(n * 64, 64), 64), :], dx1[...])
        dwp[n, DB_ROW:G_ROWS, 0:256] = jnp.broadcast_to(
            jnp.sum(dza[n].astype(F32), axis=0, keepdims=True), (G_ROWS - DB_ROW, 256))
        dwp[n, DB_ROW:G_ROWS, 256:512] = jnp.zeros((G_ROWS - DB_ROW, 256), F32)

    def pair_copy(i):
        return rc(dwp.at[2 * i + 1 - core], dwr.at[i], dw_ss.at[i], dw_rs.at[i], PT)

    @pl.loop(0, chips)
    def _(i):
        grads(2 * i + 1 - core)
        pair_copy(i).start()

    @pl.loop(0, chips)
    def _(i):
        grads(2 * i + core)

    acc[...] = jnp.zeros_like(acc)

    @pl.loop(0, n_dev)
    def _(n):
        for r in range(2):
            rows = slice(r * 256, r * 256 + 256)
            acc[rows, :] += mm(ga[n, rows, :], wp[n, W2_ROW:W1_ROW, :])

    y_out[...] = (x1[...].astype(F32) + acc[...] + bd[...].astype(F32)).astype(BF16)

    @pl.loop(0, chips)
    def _(i):
        pair_copy(i).wait_recv()
        dwp[2 * i + core] += dwr[i]

    top, low = pl.ds(0, G_HALF), pl.ds(G_HALF, G_HALF)

    def ring_copy(step):
        src, dst, target = (
            (dwp.at[O, top, :], r_a, R), (dwp.at[O, low, :], r_b, L), (dwp.at[R], r_l, R), (dwp.at[L], r_r, L))[step]
        return rc(src, dst, dw_ss.at[chips + step], dw_rs.at[chips + step], target)

    ring_copy(0).start()
    ring_copy(1).start()

    for j in range(n_dev):
        @pl.when(me != j)
        def _():
            do_copy(me, j).wait_recv()
        for b in range(2):
            do_t = do_all[j, :, b * 256:(b + 1) * 256].astype(F32)
            do_s[b, j * 256:(j + 1) * 256, :] = do_t.T.astype(BF16)
            delta[b, :, j * 256:(j + 1) * 256] = jnp.sum(
                do_t * o_own[b, :, j * 256:(j + 1) * 256].astype(F32), axis=0, keepdims=True)
    dqt[...] = jnp.zeros_like(dqt)
    dwqkv_out[...] = jnp.zeros_like(dwqkv_out)
    dbqkv_out[...] = jnp.zeros_like(dbqkv_out)

    def dq_copy(b, j, src):
        lanes = pl.ds(b * 256, 256)
        return rc(dqkvt.at[b, :, m256(j)], dqkvt_all.at[src, :, lanes], dq_ss.at[b, j], dq_rs.at[b, src], j)

    def tile(b, kb, qb, masked):
        rows, cols = m256(kb), m256(qb)
        s = mm(k_s[b, rows, :], qkvt[b, 0:64, cols]) * s_fac
        p = jnp.exp2(s - lse[b, :, cols])
        if masked:
            p = jnp.where(causal((256, 256)), p, 0.0)
        dp = mm(v_s[b, rows, :], do_all[qb, :, b * 256:(b + 1) * 256]).astype(BF16).astype(F32)
        ds = (p * (dp - delta[b, :, cols]) * attn_scale).astype(BF16)
        dv = mm(p.astype(BF16), do_s[b, cols, :])
        dk = mm(ds, q_s[b, cols, :])
        dqt[b, :, cols] += mm(qkvt[b, 64:128, rows], ds)
        if masked:
            dv_s[b] = dv
            dk_s[b] = dk
        else:
            dv_s[b] += dv
            dk_s[b] += dk

    @pl.loop(0, n_dev)
    def _(kb):
        @pl.when(kb == 3)
        def _():
            ring_copy(0).wait_recv()
            dwp[R, top, :] += r_a[...]
            ring_copy(2).start()
            ring_copy(1).wait_recv()
            dwp[L, low, :] += r_b[...]
            ring_copy(3).start()

        for b in range(2):
            tile(b, kb, kb, True)

        @pl.loop(kb + 1, n_dev)
        def _(qb):
            for b in range(2):
                tile(b, kb, qb, False)

        cols = m256(kb)
        for b in range(2):
            dkv_t = jnp.concatenate([dk_s[b], dv_s[b]], axis=1).T
            dqkvt[b, 0:64, cols] = dqt[b, :, cols].astype(BF16)
            dqkvt[b, 64:192, cols] = dkv_t.astype(BF16)

            @pl.when(kb != me)
            def _():
                dq_copy(b, kb, me).start()

            blk = dqkvt[b, :, cols]

            @pl.when(kb == me)
            def _():
                dqkvt_all[me, :, b * 256:(b + 1) * 256] = blk

            dwqkv_out[...] += mm(blk, h1[b, cols, :])
            dbqkv_out[...] += mm(jnp.ones((8, 256), BF16), blk, 1, 1)

    ring_copy(2).wait_recv()
    ring_copy(3).wait_recv()
    dwd_out[...] = dwp[me, W2_ROW:W1_ROW, :] + r_l[W2_ROW:W1_ROW, :] + r_r[W2_ROW:W1_ROW, :]
    dwu_out[...] = (dwp[me, W1_ROW:WO_ROW, :] + r_l[W1_ROW:WO_ROW, :] + r_r[W1_ROW:WO_ROW, :]).T
    dwo_out[...] = dwp[me, WO_ROW:DB_ROW, :] + r_l[WO_ROW:DB_ROW, :] + r_r[WO_ROW:DB_ROW, :]
    dbu_out[...] = dwp[me, DB_ROW:DB_ROW + 8, 0:256] + r_l[DB_ROW:DB_ROW + 8, 0:256] + r_r[DB_ROW:DB_ROW + 8, 0:256]

    for b in range(2):
        for src in range(n_dev):
            @pl.when(me != src)
            def _():
                dq_copy(b, me, src).wait_recv()
    acc[...] = jnp.zeros_like(acc)

    @pl.loop(0, n_dev)
    def _(n):
        for r in range(2):
            rows = slice(r * 256, r * 256 + 256)
            acc[rows, :] += mm(dqkvt_all[n, :, rows], wp[n, WQ_ROW:BU_ROW, :], 0, 0)

    for r in range(4):
        rows = slice(r * 128, r * 128 + 128)
        dh1 = acc[rows, :].astype(BF16).astype(F32)
        x_hat, inv_std = norm_stats(x[rows, :].astype(F32))
        dx_out[rows, :] = (dx1[rows, :].astype(F32) + norm_back(dh1, x_hat, inv_std, gain1)).astype(BF16)
        vec[0:1, :] += jnp.sum(dh1 * x_hat, axis=0, keepdims=True)
        vec[1:2, :] += jnp.sum(dh1, axis=0, keepdims=True)

    def vec_copy(j, src):
        return rc(vec, vec_all.at[src], v_ss.at[j], v_rs.at[src], j)

    for j in range(n_dev):
        @pl.when(me != j)
        def _():
            vec_copy(j, me).start()
    vec_all[me] = vec[...]
    for j in range(n_dev):
        @pl.when(me != j)
        def _():
            vec_copy(me, j).wait_recv()
    total = vec_all[0]
    for j in range(1, n_dev):
        total = total + vec_all[j]
    vec_out[...] = total

    for a in range(3):
        for ch in range(9):
            ag_copy(a, ch, False).wait_send()
    for i in range(chips):
        pair_copy(i).wait_send()
    for step in range(4):
        ring_copy(step).wait_send()
    for j in range(n_dev):
        @pl.when(me != j)
        def _():
            do_copy(j, me).wait_send()
            vec_copy(j, me).wait_send()
            for b in range(2):
                o_copy(b, j, me).wait_send()
                dq_copy(b, j, me).wait_send()


def solution(mesh):
    n_dev = mesh.shape["tp"]

    def device_step(hidden, grad_out, ln1_gain, ln1_bias, w_qkv, b_qkv, w_out, b_out, ln2_gain, ln2_bias, w_up, b_up, w_down, b_down):
        batch, tokens, d = hidden.shape
        rows = batch * tokens
        head = w_qkv.shape[-1]
        seq = tokens * n_dev
        ff = w_up.shape[1]
        attn_scale = head ** -0.5
        row = lambda v: v.reshape(1, -1)
        wq = jnp.pad(w_qkv.reshape(d, 3 * head), ((0, 0), (0, 256 - 3 * head)))
        bq = jnp.pad(b_qkv.reshape(1, 3 * head), ((0, 0), (0, 256 - 3 * head)))
        sds = jax.ShapeDtypeStruct
        vm = pltpu.VMEM
        dma = pltpu.SemaphoreType.DMA
        outs = pl.pallas_call(
            lambda *refs: layer_kernel(n_dev, attn_scale, *refs),
            out_shape=(sds((rows, d), BF16), sds((rows, d), BF16), sds((8, d), F32), sds((3 * head, d), F32), sds((8, 3 * head), F32),
                       sds((head, d), F32), sds((d, ff), F32), sds((8, ff), F32), sds((ff, d), F32)),
            in_specs=[pl.BlockSpec(memory_space=pltpu.VMEM)] * 14,
            out_specs=tuple([pl.BlockSpec(memory_space=pltpu.VMEM)] * 9),
            scratch_shapes=[
                vm((2, seq, d), BF16), vm((n_dev, W_ROWS, d), BF16),
                vm((2, seq, head), BF16), vm((2, seq, head), BF16), vm((2, seq, head), BF16), vm((2, 3 * head, seq), BF16),
                vm((seq, 256), F32), vm((2, 1, seq), F32), vm((2, head, seq), BF16), vm((n_dev * head, rows), BF16),
                vm((n_dev * head, d), BF16), vm((rows, d), BF16), vm((rows, d), BF16),
                vm((n_dev, rows, ff), BF16), vm((n_dev, rows, ff), BF16), vm((rows, d), F32), vm((rows, d), BF16),
                vm((n_dev * head, rows), BF16), vm((n_dev, head, rows), BF16), vm((2, seq, head), BF16),
                vm((2, 1, seq), F32), vm((2, head, seq), F32), vm((2, 256, head), F32), vm((2, 256, head), F32),
                vm((2, 3 * head, seq), BF16), vm((n_dev, 3 * head, rows), BF16),
                vm((n_dev, G_ROWS, d), F32), vm((n_dev // 2, G_ROWS, d), F32),
                vm((G_HALF, d), F32), vm((G_HALF, d), F32), vm((G_ROWS, d), F32), vm((G_ROWS, d), F32),
                vm((8, d), F32), vm((n_dev, 8, d), F32),
                dma((3, 9)), dma((3, 9)), dma((2, n_dev)), dma((2, n_dev)), dma((n_dev,)), dma((n_dev,)),
                dma((2, n_dev)), dma((2, n_dev)), dma((n_dev // 2 + 4,)), dma((n_dev // 2 + 4,)), dma((n_dev,)), dma((n_dev,)),
            ],
            compiler_params=pltpu.CompilerParams(collective_id=0, has_side_effects=True, vmem_limit_bytes=67043328),
            name="layer",
        )(hidden.reshape(rows, d), grad_out.reshape(rows, d), row(ln1_gain), row(ln1_bias), row(b_out), row(ln2_gain), row(ln2_bias),
          row(b_down), wq, bq, w_out.reshape(head, d), w_up, row(b_up), w_down)
        y, dx, vec, dwqkv_t, dbqkv, dwo, dwu, dbu, dwd = outs
        return (y.reshape(hidden.shape), dx.reshape(hidden.shape), vec[0], vec[1], dwqkv_t.T.reshape(w_qkv.shape),
                dbqkv[0].reshape(b_qkv.shape), dwo.reshape(w_out.shape), vec[2], vec[3], vec[4], dwu, dbu[0], dwd, vec[5])

    act_spec = P("dp", "tp", None)
    vec_spec = P(None)
    group_vec = P("dp")
    in_specs = (act_spec, act_spec, vec_spec, vec_spec, P(None, None, "tp", None), P(None, "tp", None), P("tp", None, None), vec_spec, vec_spec, vec_spec, P(None, "tp"), P("tp"), P("tp", None), vec_spec)
    out_specs = (act_spec, act_spec, group_vec, group_vec, P("dp", None, "tp", None), P("dp", "tp", None), P(("dp", "tp"), None, None), group_vec, group_vec, group_vec, P("dp", "tp"), P(("dp", "tp")), P(("dp", "tp"), None), group_vec)
    return jax.shard_map(device_step, mesh=mesh, in_specs=in_specs, out_specs=out_specs, check_vma=False)
```

```python
import jax
import jax.numpy as jnp
from jax import lax
from jax.experimental import pallas as pl
from jax.experimental.pallas import tpu as pltpu
from jax.sharding import PartitionSpec as P

LN_EPS = 1e-5
MESH = pl.DeviceIdType.MESH
F32 = jnp.float32
BF16 = jnp.bfloat16
LOG2E = 1.4426950408889634
GELU_A = 0.7978845608028654
GELU_B = 0.044715

W_ROWS, WO_ROWS = 512, 80
GB_ROWS = 336


def mm(lhs, rhs, lc=1, rc=0):
    return lax.dot_general(lhs, rhs, (((lc,), (rc,)), ((), ())), preferred_element_type=F32)


def norm_stats(value):
    centered = value - jnp.mean(value, axis=-1, keepdims=True)
    inv_std = lax.rsqrt(jnp.mean(centered * centered, axis=-1, keepdims=True) + LN_EPS)
    return centered * inv_std, inv_std


def norm_back(grad, x_hat, inv_std, gain):
    scaled = grad * gain
    return inv_std * (scaled - jnp.mean(scaled, axis=-1, keepdims=True) - x_hat * jnp.mean(scaled * x_hat, axis=-1, keepdims=True))


def vector(ref):
    return ref[...].astype(F32).reshape(1, -1)


def layer_kernel(n_dev, attn_scale,
                 x, dy, g1, s1, bo, g2, s2, bd, wqkv, bqkv, wo, wu, bu, wd,
                 y_out, dx_out, vec_out, dwqkv_out, dwo_out, dwu_out, dbu_out, dwd_out,
                 h1own, h1, wob, wp, wqp, wq, q_s, k_s, v_s, qkvt, big, lse, o_own, o_all, wo_all, x1, h2, ga, dza, acc, dx1,
                 do_send, do_all, do_s, delta, dqt, dqkvt, dh_send, dh_pair, dh_all, dwq, dwq_r,
                 dwa, dwb, pra, prb, ra_a, ra_b, ra_l, ra_r, rb_a, rb_b, rb_l, rb_r, vec, vec_all,
                 hs_ss, hs_rs, hp_ss, hp_rs, wq_ss, wq_rs, ag_ss, ag_rs, o_ss, o_rs, do_ss, do_rs, dhp_ss, dhp_rs, dh_ss, dh_rs,
                 pr_ss, pr_rs, rg_ss, rg_rs, v_ss, v_rs):
    me = lax.axis_index("tp")
    chips = n_dev // 2
    chip, core = lax.div(me, 2), lax.rem(me, 2)
    seq = lax.div(chip, chips // 2)
    mate = 2 * (chips - 1 - chip) + core

    def dev(shift, other):
        return 2 * lax.rem(chip + shift + chips, chips) + (1 - core if other else core)

    L, R, O, PT = dev(-1, False), dev(1, False), dev(2, False), dev(0, True)
    PL, PR, PO = dev(-1, True), dev(1, True), dev(2, True)

    def handler(n, st):
        return n if (n // 2) // (chips // 2) == st else 2 * (chips - 1 - n // 2) + n % 2

    def rc(src, dst, ssem, rsem, target):
        return pltpu.make_async_remote_copy(src_ref=src, dst_ref=dst, send_sem=ssem, recv_sem=rsem,
                                            device_id={"tp": target}, device_id_type=MESH)

    def m256(i):
        return pl.ds(i * 256, 256) if isinstance(i, int) else pl.ds(pl.multiple_of(i * 256, 256), 256)

    def m64(i):
        return pl.ds(i * 64, 64) if isinstance(i, int) else pl.ds(pl.multiple_of(i * 64, 64), 64)

    plan = ((me, "F", R, L), (me, "F", L, R), (me, "F", PT, PT), (L, "A", R, O), (R, "B", L, O),
            (L, "F", PT, PL), (R, "F", PT, PR), (O, "A", PT, PO), (O, "B", PT, PO))

    def view(a, owner, part):
        cut, rows = ((48, WO_ROWS), (256, W_ROWS))[a]
        off, size = {"F": (0, rows), "A": (0, cut), "B": (cut, rows - cut)}[part]
        return (wob, wp)[a].at[owner, pl.ds(off, size), :]

    def ag_copy(a, ch, received):
        own, part, target, got = plan[ch]
        v = view(a, got if received else own, part)
        return rc(v, v, ag_ss.at[a, ch], ag_rs.at[a, ch], target)

    def ag_start(a, *chs):
        for ch in chs:
            ag_copy(a, ch, False).start()

    def ag_wait(a, *chs):
        for ch in chs:
            ag_copy(a, ch, True).wait_recv()

    barrier = pltpu.get_barrier_semaphore()
    for i in range(n_dev):
        @pl.when(me != i)
        def _():
            pl.semaphore_signal(barrier, inc=1, device_id={"tp": i}, device_id_type=MESH)

    gain1, shift1 = vector(g1), vector(s1)
    for b in range(2):
        for r in range(2):
            rows = slice(b * 256 + r * 128, b * 256 + r * 128 + 128)
            x_hat, _ = norm_stats(x[rows, :].astype(F32))
            h1own[b, r * 128:r * 128 + 128, :] = (x_hat * gain1 + shift1).astype(BF16)
    h1[m256(me), :] = h1own[seq]
    wqp[0, 0:192, :] = wqkv[...]
    bq_row = jnp.concatenate([bqkv[c].astype(F32) for c in range(3)] + [jnp.zeros((1, 320), F32)], axis=1)
    wqp[0, 192:208, :] = jnp.broadcast_to(bq_row, (16, 512)).astype(BF16)

    def h1_send(t):
        return rc(h1own.at[t // (chips // 2)], h1.at[m256(me), :], hs_ss.at[t], hs_rs.at[chip], 2 * t + core)

    def h1_recv(src):
        return rc(h1own.at[0], h1.at[m256(2 * src + core), :], hs_ss.at[0], hs_rs.at[src], PT)

    def h1_pair(src, received):
        rows = m256(2 * src + (1 - core if received else core))
        return rc(h1.at[rows, :], h1.at[rows, :], hp_ss.at[src], hp_rs.at[src], PT)

    def wq_copy():
        return rc(wqp.at[0], wqp.at[1], wq_ss.at[0], wq_rs.at[0], mate)

    pl.semaphore_wait(barrier, n_dev - 1)
    wq_copy().start()
    for t in range(chips):
        @pl.when(chip != t)
        def _():
            h1_send(t).start()
    h1_pair(chip, False).start()

    wob[me, 0:64, :] = wo[...]
    wob[me, 64:80, 0:256] = jnp.broadcast_to(vector(bu), (16, 256)).astype(BF16)
    wob[me, 64:80, 256:512] = jnp.zeros((16, 256), BF16)
    wp[me, 0:256, :] = wd[...]
    wp[me, 256:512, :] = wu[...].astype(F32).T.astype(BF16)

    def natural(hi):
        full = jnp.concatenate([wqp[hi, 0:192, :].astype(F32), jnp.zeros((64, 512), F32)], axis=0)
        wq[:, hi * 256:(hi + 1) * 256] = full.T.astype(BF16)

    natural(0)
    wq_copy().wait_recv()
    natural(1)
    bias_qkv = jnp.concatenate([wqp[hi, 192:208, 0:256].astype(F32)[0:1, :] for hi in range(2)], axis=1)

    def project(owner):
        rows = m256(owner)
        full = (mm(h1[rows, :], wq[...]) + bias_qkv).astype(BF16).astype(F32)
        for hi in range(2):
            part = full[:, hi * 256:(hi + 1) * 256]
            q_s[hi, rows, :] = part[:, 0:64].astype(BF16)
            k_s[hi, rows, :] = part[:, 64:128].astype(BF16)
            v_s[hi, rows, :] = part[:, 128:192].astype(BF16)
            qkvt[hi, :, rows] = part.T[:192, :].astype(BF16)

    @pl.loop(0, chips)
    def _(t):
        src = lax.rem(chip + t + lax.div(t, 2) - 2 * lax.div(t, 3), chips)

        @pl.when(t > 0)
        def _():
            h1_recv(src).wait_recv()
            h1_pair(src, False).start()

        project(2 * src + core)
        h1_pair(src, True).wait_recv()
        project(2 * src + 1 - core)

    for a in range(2):
        ag_start(a, 0, 1, 2)

    s_fac = attn_scale * LOG2E
    keep = lax.broadcasted_iota(jnp.int32, (256, 256), 0) <= lax.broadcasted_iota(jnp.int32, (256, 256), 1)

    def o_copy(hi, j):
        head = me + hi * (mate - me)
        return rc(o_own.at[hi, :, m256(j)], o_all.at[m64(head), m256(seq)], o_ss.at[hi, j], o_rs.at[seq, head], j)

    def fold(value, op):
        return op(value.reshape(32, 8, 256), axis=0)

    def attend(hi, j):
        cols = m256(j)
        q_t = qkvt[hi, 0:64, cols]
        base = 8 * (j % 2)
        m = jnp.full((8, 256), -1e30, F32)
        for kc in range(j + 1):
            s = mm(k_s[hi, m256(kc), :], q_t) * s_fac
            if kc == j:
                s = jnp.where(keep, s, -1e30)
            big[base + kc] = s
            m = jnp.maximum(m, fold(s, jnp.max))
        m = jnp.max(m, axis=0, keepdims=True)
        l = jnp.zeros((8, 256), F32)
        for kc in range(j + 1):
            l = l + fold(jnp.exp2(big[base + kc] - m), jnp.sum)
        lse_j = m + jnp.log2(jnp.sum(l, axis=0, keepdims=True))
        lse[hi, :, cols] = lse_j
        o = jnp.zeros((64, 256), F32)
        for kc in range(j + 1):
            p = jnp.exp2(big[base + kc] - lse_j).astype(BF16)
            o = o + mm(qkvt[hi, 128:192, m256(kc)], p)
        o = o.astype(BF16)
        o_own[hi, :, cols] = o

        @pl.when(me != j)
        def _():
            o_copy(hi, j).start()

        @pl.when(me == j)
        def _():
            o_all[m64(me + hi * (mate - me)), m256(seq)] = o

    @pl.loop(0, 2)
    def _(hi):
        @pl.when(hi == 1)
        def _():
            ag_wait(0, 0, 1, 2)
            ag_start(0, 3, 4, 5, 6)

        for j in range(n_dev):
            attend(hi, j)

    ag_wait(1, 0)
    ag_start(1, 3, 5)
    ag_wait(1, 1)
    ag_start(1, 4, 6)
    ag_wait(0, 3, 4)
    ag_start(0, 7, 8)
    ag_wait(0, 5, 6, 7, 8)
    for n in range(n_dev):
        wo_all[n * 64:(n + 1) * 64, :] = wob[n, 0:64, :]
    for st in range(2):
        for n in range(n_dev):
            @pl.when(me != handler(n, st))
            def _():
                rc(o_own.at[0, :, m256(0)], o_all.at[m64(n), m256(st)], o_ss.at[0, 0], o_rs.at[st, n], PT).wait_recv()

    bias_o = vector(bo)
    gain2, shift2 = vector(g2), vector(s2)
    for r in range(4):
        rows = slice(r * 128, r * 128 + 128)
        attn = mm(o_all[:, rows], wo_all[...], 0, 0)
        x1_r = (x[rows, :].astype(F32) + attn + bias_o).astype(BF16)
        x1[rows, :] = x1_r
        x_hat, _ = norm_stats(x1_r.astype(F32))
        h2[rows, :] = (x_hat * gain2 + shift2).astype(BF16)
    acc[...] = jnp.zeros_like(acc)

    packs = ((dwa, pra, ra_a, ra_b, ra_l, ra_r, 128), (dwb, prb, rb_a, rb_b, rb_l, rb_r, GB_ROWS // 2))

    def pair_copy(g, slot):
        return rc(packs[g][0].at[2 * slot + 1 - core], packs[g][1].at[slot], pr_ss.at[g, slot], pr_rs.at[g, slot], PT)

    def pair_add(g, slot):
        pair_copy(g, slot).wait_recv()
        packs[g][0][2 * slot + core] += packs[g][1][slot]

    def ring_copy(g, step):
        pack, _, r_a, r_b, r_l, r_r, half = packs[g]
        top, low = pl.ds(0, half), pl.ds(half, half)
        src, dst, target = (
            (pack.at[O, top, :], r_a, R), (pack.at[O, low, :], r_b, L), (pack.at[R], r_l, R), (pack.at[L], r_r, L))[step]
        return rc(src, dst, rg_ss.at[g, step], rg_rs.at[g, step], target)

    def ring_begin(g):
        pair_add(g, lax.rem(chip + 2, chips))
        ring_copy(g, 0).start()
        ring_copy(g, 1).start()
        for shift in (1, 3, 0):
            pair_add(g, lax.rem(chip + shift, chips))

    def ring_turn(g):
        pack, _, r_a, r_b, _, _, half = packs[g]
        ring_copy(g, 0).wait_recv()
        pack[R, 0:half, :] += r_a[...]
        ring_copy(g, 2).start()
        ring_copy(g, 1).wait_recv()
        pack[L, half:2 * half, :] += r_b[...]
        ring_copy(g, 3).start()

    @pl.loop(0, n_dev)
    def _(i):
        t, other = lax.div(i, 2), lax.rem(i, 2)
        slot = lax.rem(chip + t + lax.div(t, 2) - 2 * lax.div(t, 3), chips)
        n = 2 * slot + core + other * (1 - 2 * core)

        @pl.when(i == 1)
        def _():
            ag_wait(1, 2)

        @pl.when(i == 3)
        def _():
            ag_wait(1, 6)

        @pl.when(i == 5)
        def _():
            ag_wait(1, 5)

        @pl.when(i == 6)
        def _():
            ag_wait(1, 3)
            ag_start(1, 7)
            ag_wait(1, 4)
            ag_start(1, 8)

        @pl.when(i == 7)
        def _():
            ag_wait(1, 7, 8)

        w2 = wp[n, 0:256, :]
        w1t = wp[n, 256:512, :]
        bias_u = wob[n, 64:80, 0:256].astype(F32)[0:1, :]
        for r in range(2):
            rows = slice(r * 256, r * 256 + 256)
            z = (mm(h2[rows, :], w1t, 1, 1) + bias_u).astype(BF16).astype(F32)
            z2 = z * z
            th = jnp.tanh(GELU_A * (z + GELU_B * z2 * z))
            ga[n, rows, :] = (0.5 * z * (1.0 + th)).astype(BF16)
            slope = 0.5 * (1.0 + th) + 0.5 * z * (1.0 - th * th) * (GELU_A * (1.0 + 3.0 * GELU_B * z2))
            dgl = mm(dy[rows, :], w2, 1, 1).astype(BF16).astype(F32)
            dz = (dgl * slope).astype(BF16)
            dza[n, rows, :] = dz
            acc[rows, :] += mm(dz, w1t)
        dwa[n] = mm(ga[n], dy[...], 0, 0)

        @pl.when(other == 1)
        def _():
            pair_copy(0, slot).start()

    ring_begin(0)

    vec[...] = jnp.zeros_like(vec)
    for r in range(4):
        rows = slice(r * 128, r * 128 + 128)
        dh2 = acc[rows, :].astype(BF16).astype(F32)
        x_hat, inv_std = norm_stats(x1[rows, :].astype(F32))
        dy_r = dy[rows, :].astype(F32)
        dx1_r = (dy_r + norm_back(dh2, x_hat, inv_std, gain2)).astype(BF16)
        dx1[rows, :] = dx1_r
        vec[2:3, :] += jnp.sum(dx1_r.astype(F32), axis=0, keepdims=True)
        vec[3:4, :] += jnp.sum(dh2 * x_hat, axis=0, keepdims=True)
        vec[4:5, :] += jnp.sum(dh2, axis=0, keepdims=True)
        vec[5:6, :] += jnp.sum(dy_r, axis=0, keepdims=True)

    def do_copy(n, st):
        target = handler(n, st)
        hi = 0 if target == n else 1
        return rc(do_send.at[m64(n), m256(st)], do_all.at[hi, :, m256(me)], do_ss.at[n, st], do_rs.at[hi, me], target)

    for r in range(2):
        rows = slice(r * 256, r * 256 + 256)
        do_send[rows, :] = mm(wo_all[rows, :], dx1[...], 1, 1).astype(BF16)
    for n in range(n_dev):
        for st in range(2):
            @pl.when(me != handler(n, st))
            def _():
                do_copy(n, st).start()

            @pl.when(me == handler(n, st))
            def _():
                do_all[0 if handler(n, st) == n else 1, :, m256(me)] = do_send[m64(n), m256(st)]

    @pl.loop(0, n_dev)
    def _(i):
        t, other = lax.div(i, 2), 1 - lax.rem(i, 2)
        slot = lax.rem(chip + 2 + t, chips)
        n = 2 * slot + core + other * (1 - 2 * core)
        dwb[n, 0:256, :] = mm(dza[n], h2[...], 0, 0)
        dwb[n, 256:320, :] = mm(o_all[m64(n), :], dx1[...])
        dwb[n, 320:336, 0:256] = jnp.broadcast_to(jnp.sum(dza[n].astype(F32), axis=0, keepdims=True), (16, 256))
        dwb[n, 320:336, 256:512] = jnp.zeros((16, 256), F32)

        @pl.when(other == 1)
        def _():
            pair_copy(1, slot).start()

    ring_turn(0)
    ring_begin(1)

    for j in range(n_dev):
        for hi in range(2):
            @pl.when(me != j)
            def _():
                rc(do_send.at[m64(0), m256(0)], do_all.at[hi, :, m256(j)], do_ss.at[0, 0], do_rs.at[hi, j], PT).wait_recv()
            do_t = do_all[hi, :, m256(j)].astype(F32)
            do_s[hi, m256(j), :] = do_t.T.astype(BF16)
            delta[hi, :, m256(j)] = jnp.sum(do_t * o_own[hi, :, m256(j)].astype(F32), axis=0, keepdims=True)
    dwq[...] = jnp.zeros_like(dwq)

    def dwq_copy():
        return rc(dwq.at[1], dwq_r, wq_ss.at[1], wq_rs.at[1], mate)

    def dh_pair_copy(kb):
        return rc(dh_send.at[kb], dh_pair.at[kb // 2], dhp_ss.at[kb // 2], dhp_rs.at[kb // 2], PT)

    def dh_copy(kb):
        return rc(dh_send.at[kb], dh_all.at[chip], dh_ss.at[kb // 2], dh_rs.at[chip], kb)

    def dh_finish(kb):
        @pl.when(core == kb % 2)
        def _():
            dh_pair_copy(kb).wait_recv()
            total = (dh_send[kb].astype(F32) + dh_pair[kb // 2].astype(F32)).astype(BF16)
            dh_send[kb] = total

            @pl.when(me != kb)
            def _():
                dh_copy(kb).start()

            @pl.when(me == kb)
            def _():
                dh_all[chip] = total

    @pl.loop(0, 2)
    def _(i):
        hi = 1 - i

        @pl.when(i == 1)
        def _():
            dwq_copy().start()

        for kb in range(n_dev):
            rows = m256(kb)
            k_b, v_b, kt_b = k_s[hi, rows, :], v_s[hi, rows, :], qkvt[hi, 64:128, rows]
            dk = jnp.zeros((256, 64), F32)
            dv = jnp.zeros((256, 64), F32)
            for qb in range(kb, n_dev):
                cols = m256(qb)
                p = jnp.exp2(mm(k_b, qkvt[hi, 0:64, cols]) * s_fac - lse[hi, :, cols])
                if qb == kb:
                    p = jnp.where(keep, p, 0.0)
                dp = mm(v_b, do_all[hi, :, cols]).astype(BF16).astype(F32)
                ds = (p * (dp - delta[hi, :, cols]) * attn_scale).astype(BF16)
                dv = dv + mm(p.astype(BF16), do_s[hi, cols, :])
                dk = dk + mm(ds, q_s[hi, cols, :])
                dq = mm(kt_b, ds)
                if kb == 0:
                    dqt[:, cols] = dq
                else:
                    dqt[:, cols] += dq
            dqkvt[hi, 0:64, rows] = dqt[:, rows].astype(BF16)
            dqkvt[hi, 64:192, rows] = jnp.concatenate([dk, dv], axis=1).T.astype(BF16)
            blk = dqkvt[hi, :, rows]
            dwq[hi, 0:192, :] += mm(blk, h1[rows, :])
            dwq[hi, 192:200, 0:192] += mm(jnp.ones((8, 256), BF16), blk, 1, 1)

            @pl.when(i == 1)
            def _():
                dh = mm(dqkvt[0, :, rows], wqp[0, 0:192, :], 0, 0) + mm(dqkvt[1, :, rows], wqp[1, 0:192, :], 0, 0)
                dh_send[kb] = dh.astype(BF16)

                @pl.when(core != kb % 2)
                def _():
                    dh_pair_copy(kb).start()

                if kb > 0:
                    dh_finish(kb - 1)

            if kb == 2:
                @pl.when(i == 0)
                def _():
                    ring_turn(1)

    dh_finish(n_dev - 1)

    for g in range(2):
        ring_copy(g, 2).wait_recv()
        ring_copy(g, 3).wait_recv()
    dwd_out[...] = dwa[me] + ra_l[...] + ra_r[...]
    dwu_out[...] = (dwb[me, 0:256, :] + rb_l[0:256, :] + rb_r[0:256, :]).T
    dwo_out[...] = dwb[me, 256:320, :] + rb_l[256:320, :] + rb_r[256:320, :]
    dbu_out[...] = dwb[me, 320:328, 0:256] + rb_l[320:328, 0:256] + rb_r[320:328, 0:256]

    acc[...] = jnp.zeros_like(acc)

    @pl.loop(0, n_dev)
    def _(n):
        for r in range(2):
            rows = slice(r * 256, r * 256 + 256)
            acc[rows, :] += mm(ga[n, rows, :], wp[n, 0:256, :])

    y_out[...] = (x1[...].astype(F32) + acc[...] + vector(bd)).astype(BF16)

    for t in range(chips):
        @pl.when(chip != t)
        def _():
            rc(dh_send.at[0], dh_all.at[t], dh_ss.at[0], dh_rs.at[t], PT).wait_recv()

    for r in range(4):
        rows = slice(r * 128, r * 128 + 128)
        half = slice((r % 2) * 128, (r % 2) * 128 + 128)
        first = (r // 2) * (chips // 2)
        dh1 = (dh_all[first, half, :].astype(F32) + dh_all[first + 1, half, :].astype(F32)).astype(BF16).astype(F32)
        x_hat, inv_std = norm_stats(x[rows, :].astype(F32))
        dx_out[rows, :] = (dx1[rows, :].astype(F32) + norm_back(dh1, x_hat, inv_std, gain1)).astype(BF16)
        vec[0:1, :] += jnp.sum(dh1 * x_hat, axis=0, keepdims=True)
        vec[1:2, :] += jnp.sum(dh1, axis=0, keepdims=True)

    def vec_copy(j):
        return rc(vec, vec_all.at[me], v_ss.at[j], v_rs.at[me], j)

    for j in range(n_dev):
        @pl.when(me != j)
        def _():
            vec_copy(j).start()
    vec_all[me] = vec[...]
    dwq_copy().wait_recv()
    dwqkv_out[...] = dwq[0] + dwq_r[...]
    for j in range(n_dev):
        @pl.when(me != j)
        def _():
            rc(vec, vec_all.at[j], v_ss.at[0], v_rs.at[j], PT).wait_recv()
    total = vec_all[0]
    for j in range(1, n_dev):
        total = total + vec_all[j]
    vec_out[...] = total

    wq_copy().wait_send()
    dwq_copy().wait_send()
    for t in range(chips):
        h1_pair(t, False).wait_send()

        @pl.when(chip != t)
        def _():
            h1_send(t).wait_send()
        for g in range(2):
            pair_copy(g, t).wait_send()
    for a in range(2):
        for ch in range(9):
            ag_copy(a, ch, False).wait_send()
    for g in range(2):
        for step in range(4):
            ring_copy(g, step).wait_send()
    for j in range(n_dev):
        @pl.when(me != j)
        def _():
            vec_copy(j).wait_send()
            for hi in range(2):
                o_copy(hi, j).wait_send()

        for st in range(2):
            @pl.when(me != handler(j, st))
            def _():
                do_copy(j, st).wait_send()

        @pl.when(core != j % 2)
        def _():
            dh_pair_copy(j).wait_send()

        @pl.when((core == j % 2) & (me != j))
        def _():
            dh_copy(j).wait_send()


def finish_kernel(y, dx, vec, dwqkv, dwo, dwu, dbu, dwd, y_o, dx_o, v0, v1, dwqkv_o, dbqkv_o, dwo_o, v2, v3, v4, dwu_o, dbu_o, dwd_o, v5):
    y_o[...] = y[...]
    dx_o[...] = dx[...]
    for i, ref in enumerate((v0, v1, v2, v3, v4, v5)):
        ref[...] = vec[i:i + 1, :].reshape(ref.shape)
    dwqkv_o[...] = dwqkv[0:192, :]
    for c in range(3):
        dbqkv_o[c] = dwqkv[192:193, c * 64:(c + 1) * 64]
    dwo_o[...] = dwo[...]
    dwu_o[...] = dwu[...]
    dbu_o[...] = dbu[0:1, :].reshape(dbu_o.shape)
    dwd_o[...] = dwd[...]


def solution(mesh):
    n_dev = mesh.shape["tp"]

    def device_step(hidden, grad_out, ln1_gain, ln1_bias, w_qkv, b_qkv, w_out, b_out, ln2_gain, ln2_bias, w_up, b_up, w_down, b_down):
        batch, tokens, d = hidden.shape
        rows = batch * tokens
        head = w_qkv.shape[-1]
        seq = tokens * n_dev
        ff = w_up.shape[1]
        chips = n_dev // 2
        attn_scale = head ** -0.5
        sds = jax.ShapeDtypeStruct
        vm = pltpu.VMEM

        def dma(*shape):
            return pltpu.SemaphoreType.DMA(shape)

        vspec = pl.BlockSpec(memory_space=pltpu.VMEM)
        outs = pl.pallas_call(
            lambda *refs: layer_kernel(n_dev, attn_scale, *refs),
            out_shape=(sds((rows, d), BF16), sds((rows, d), BF16), sds((8, d), F32), sds((200, d), F32),
                       sds((head, d), F32), sds((d, ff), F32), sds((8, ff), F32), sds((ff, d), F32)),
            in_specs=[vspec] * 14,
            out_specs=tuple([vspec] * 8),
            scratch_shapes=[
                vm((2, tokens, d), BF16), vm((seq, d), BF16), vm((n_dev, WO_ROWS, d), BF16), vm((n_dev, W_ROWS, d), BF16),
                vm((2, 208, d), BF16), vm((d, 512), BF16),
                vm((2, seq, head), BF16), vm((2, seq, head), BF16), vm((2, seq, head), BF16), vm((2, 3 * head, seq), BF16),
                vm((16, 256, 256), F32), vm((2, 1, seq), F32), vm((2, head, seq), BF16), vm((n_dev * head, rows), BF16),
                vm((n_dev * head, d), BF16), vm((rows, d), BF16), vm((rows, d), BF16),
                vm((n_dev, rows, ff), BF16), vm((n_dev, rows, ff), BF16), vm((rows, d), F32), vm((rows, d), BF16),
                vm((n_dev * head, rows), BF16), vm((2, head, seq), BF16), vm((2, seq, head), BF16),
                vm((2, 1, seq), F32), vm((head, seq), F32), vm((2, 3 * head, seq), BF16),
                vm((n_dev, tokens, d), BF16), vm((chips, tokens, d), BF16), vm((chips, tokens, d), BF16),
                vm((2, 200, d), F32), vm((200, d), F32),
                vm((n_dev, ff, d), F32), vm((n_dev, GB_ROWS, d), F32), vm((chips, ff, d), F32), vm((chips, GB_ROWS, d), F32),
                vm((ff // 2, d), F32), vm((ff // 2, d), F32), vm((ff, d), F32), vm((ff, d), F32),
                vm((GB_ROWS // 2, d), F32), vm((GB_ROWS // 2, d), F32), vm((GB_ROWS, d), F32), vm((GB_ROWS, d), F32),
                vm((8, d), F32), vm((n_dev, 8, d), F32),
                dma(chips), dma(chips), dma(chips), dma(chips), dma(2), dma(2), dma(2, 9), dma(2, 9), dma(2, n_dev), dma(2, n_dev),
                dma(n_dev, 2), dma(2, n_dev), dma(chips), dma(chips), dma(chips), dma(chips),
                dma(2, chips), dma(2, chips), dma(2, 4), dma(2, 4), dma(n_dev), dma(n_dev),
            ],
            compiler_params=pltpu.CompilerParams(collective_id=0, has_side_effects=True, vmem_limit_bytes=67043328),
            name="layer",
        )(hidden.reshape(rows, d), grad_out.reshape(rows, d), ln1_gain, ln1_bias, b_out, ln2_gain, ln2_bias, b_down,
          w_qkv.transpose(1, 2, 3, 0).reshape(3 * head, d), b_qkv, w_out.reshape(head, d), w_up, b_up, w_down)
        v1d = sds((d,), F32)
        y, dx, v0, v1, dwqkv_t, dbqkv, dwo, v2, v3, v4, dwu, dbu, dwd, v5 = pl.pallas_call(
            finish_kernel,
            out_shape=(sds((rows, d), BF16), sds((rows, d), BF16), v1d, v1d, sds((3 * head, d), F32), sds((3, 1, head), F32),
                       sds((head, d), F32), v1d, v1d, v1d, sds((d, ff), F32), sds((ff,), F32), sds((ff, d), F32), v1d),
            in_specs=[vspec] * 8,
            out_specs=tuple([vspec] * 14),
            name="finish",
        )(*outs)
        return (y.reshape(hidden.shape), dx.reshape(hidden.shape), v0, v1, dwqkv_t.reshape(3, 1, head, d).transpose(3, 0, 1, 2),
                dbqkv, dwo.reshape(w_out.shape), v2, v3, v4, dwu, dbu, dwd, v5)

    act_spec = P("dp", "tp", None)
    vec_spec = P(None)
    group_vec = P("dp")
    in_specs = (act_spec, act_spec, vec_spec, vec_spec, P(None, None, "tp", None), P(None, "tp", None), P("tp", None, None), vec_spec, vec_spec, vec_spec, P(None, "tp"), P("tp"), P("tp", None), vec_spec)
    out_specs = (act_spec, act_spec, group_vec, group_vec, P("dp", None, "tp", None), P("dp", "tp", None), P(("dp", "tp"), None, None), group_vec, group_vec, group_vec, P("dp", "tp"), P(("dp", "tp")), P(("dp", "tp"), None), group_vec)
    return jax.shard_map(device_step, mesh=mesh, in_specs=in_specs, out_specs=out_specs, check_vma=False)
```

```python
import jax
import jax.numpy as jnp
from jax import lax
from jax.experimental import pallas as pl
from jax.experimental.pallas import tpu as pltpu
from jax.sharding import PartitionSpec as P

LN_EPS = 1e-5
MESH = pl.DeviceIdType.MESH
F32 = jnp.float32
BF16 = jnp.bfloat16
LOG2E = 1.4426950408889634
GELU_A = 0.7978845608028654
GELU_B = 0.044715

WO_ROWS = 80
G_ROWS = 528


def mm(lhs, rhs, lc=1, rc=0):
    return lax.dot_general(lhs, rhs, (((lc,), (rc,)), ((), ())), preferred_element_type=F32)


def norm_stats(value):
    centered = value - jnp.mean(value, axis=-1, keepdims=True)
    inv_std = lax.rsqrt(jnp.mean(centered * centered, axis=-1, keepdims=True) + LN_EPS)
    return centered * inv_std, inv_std


def norm_back(grad, x_hat, inv_std, gain):
    scaled = grad * gain
    return inv_std * (scaled - jnp.mean(scaled, axis=-1, keepdims=True) - x_hat * jnp.mean(scaled * x_hat, axis=-1, keepdims=True))


def vector(ref):
    return ref[...].astype(F32).reshape(1, -1)


def layer_kernel(n_dev, attn_scale,
                 x, dy, g1, s1, bo, g2, s2, bd, wqkv, bqkv, wo, wu, bu, wd,
                 y_out, dx_out, vec_out, dwqkv_out, dwo_out, dwu_out, dbu_out, dwd_out,
                 h1own, h1, wob, wp, wqp, wq, q_s, k_s, v_s, qkvt, big, lse, o_own, o_all, wo_all, x1, hh, dyy, ga, dza, acc, dx1,
                 do_send, do_all, do_s, delta, dqt, dqkvt, dh_send, dh_pair, dh_all, dwq, dwq_r,
                 dwp, prx, frx, dwop, dwo_pr, dwo_rx, vec, vec_all,
                 hs_ss, hs_rs, hp_ss, hp_rs, wq_ss, wq_rs, wb_ss, wb_rs, o_ss, o_rs, do_ss, do_rs, dhp_ss, dhp_rs, dh_ss, dh_rs,
                 wp_ss, wp_rs, mt_ss, mt_rs, pr_ss, pr_rs, fr_ss, fr_rs, op_ss, op_rs, ox_ss, ox_rs, v_ss, v_rs):
    me = lax.axis_index("tp")
    chips = n_dev // 2
    chip, core = lax.div(me, 2), lax.rem(me, 2)
    seq = lax.div(chip, chips // 2)
    mate = 2 * (chips - 1 - chip) + core
    side = chip + 1 - 2 * lax.rem(chip, 2)
    flank, across = 2 * side + core, 2 * (chips - 1 - side) + core

    def dev(shift, other):
        return 2 * lax.rem(chip + shift + chips, chips) + (1 - core if other else core)

    PT = dev(0, True)

    def handler(n, st):
        return n if (n // 2) // (chips // 2) == st else 2 * (chips - 1 - n // 2) + n % 2

    def rc(src, dst, ssem, rsem, target):
        return pltpu.make_async_remote_copy(src_ref=src, dst_ref=dst, send_sem=ssem, recv_sem=rsem,
                                            device_id={"tp": target}, device_id_type=MESH)

    def m256(i):
        return pl.ds(i * 256, 256) if isinstance(i, int) else pl.ds(pl.multiple_of(i * 256, 256), 256)

    def m64(i):
        return pl.ds(i * 64, 64) if isinstance(i, int) else pl.ds(pl.multiple_of(i * 64, 64), 64)

    barrier = pltpu.get_barrier_semaphore()
    for i in range(n_dev):
        @pl.when(me != i)
        def _():
            pl.semaphore_signal(barrier, inc=1, device_id={"tp": i}, device_id_type=MESH)

    gain1, shift1 = vector(g1), vector(s1)
    for b in range(2):
        for r in range(2):
            rows = slice(b * 256 + r * 128, b * 256 + r * 128 + 128)
            x_hat, _ = norm_stats(x[rows, :].astype(F32))
            h1own[b, r * 128:r * 128 + 128, :] = (x_hat * gain1 + shift1).astype(BF16)
    h1[m256(me), :] = h1own[seq]
    wqp[0, 0:192, :] = wqkv[...]
    bq_row = jnp.concatenate([bqkv[c].astype(F32) for c in range(3)] + [jnp.zeros((1, 320), F32)], axis=1)
    wqp[0, 192:208, :] = jnp.broadcast_to(bq_row, (16, 512)).astype(BF16)

    def h1_copy(step):
        src, row, target = ((h1own.at[1 - seq], me, mate), (h1own.at[seq], me, flank), (h1.at[m256(mate), :], mate, flank))[step]
        return rc(src, h1.at[m256(row), :], hs_ss.at[step], hs_rs.at[step], target)

    def h1_recv(step, src):
        return rc(h1own.at[0], h1.at[m256(2 * src + core), :], hs_ss.at[0], hs_rs.at[step], PT)

    def h1_pair(src, received):
        rows = m256(2 * src + (1 - core if received else core))
        return rc(h1.at[rows, :], h1.at[rows, :], hp_ss.at[src], hp_rs.at[src], PT)

    def wq_copy():
        return rc(wqp.at[0], wqp.at[1], wq_ss.at[0], wq_rs.at[0], mate)

    pl.semaphore_wait(barrier, n_dev - 1)
    h1_copy(0).start()
    h1_copy(1).start()
    h1_pair(chip, False).start()

    wob[me, 0:64, :] = wo[...]
    wob[me, 64:80, 0:256] = jnp.broadcast_to(vector(bu), (16, 256)).astype(BF16)
    wob[me, 64:80, 256:512] = jnp.zeros((16, 256), BF16)
    wp[me, 0:256, :] = wd[...]
    wp[me, 256:512, :] = wu[...].astype(F32).T.astype(BF16)
    dyy[0:512, :] = dy[...]

    def twin(d):
        return d + 1 - 2 * core

    w_plan = ((me, PT, PT, 0, 512), (me, mate, mate, 0, 256), (me, mate, mate, 256, 256), (me, flank, flank, 0, 512),
              (mate, flank, across, 0, 256), (mate, flank, across, 256, 256),
              (flank, PT, twin(flank), 0, 512), (mate, PT, twin(mate), 0, 512), (across, PT, twin(across), 0, 512))

    def w_copy(step, received=False):
        own, target, got, off, size = w_plan[step]
        v = wp.at[got if received else own, pl.ds(off, size), :]
        return rc(v, v, wp_ss.at[step], wp_rs.at[step], target)

    def w_wait(*steps):
        for step in steps:
            w_copy(step, True).wait_recv()

    def w_start(*steps):
        for step in steps:
            w_copy(step).start()

    o_plan = ((me, PT, PT), (me, mate, mate), (me, flank, flank), (mate, flank, across),
              (flank, PT, twin(flank)), (mate, PT, twin(mate)), (across, PT, twin(across)))

    def wo_all_copy(step, received=False):
        own, target, got = o_plan[step]
        v = wob.at[got if received else own]
        return rc(v, v, wb_ss.at[step], wb_rs.at[step], target)

    def wo_wait(*steps):
        for step in steps:
            wo_all_copy(step, True).wait_recv()

    def wo_start(*steps):
        for step in steps:
            wo_all_copy(step).start()

    wo_start(0)

    def mate_copy(step):
        src, dst = ((hh.at[0:256], hh.at[512:768]), (hh.at[256:512], hh.at[768:1024]), (dyy.at[0:512], dyy.at[512:1024]))[step]
        return rc(src, dst, mt_ss.at[step], mt_rs.at[step], mate)

    w_start(0)

    def natural(hi):
        full = jnp.concatenate([wqp[hi, 0:192, :].astype(F32), jnp.zeros((64, 512), F32)], axis=0)
        wq[:, hi * 256:(hi + 1) * 256] = full.T.astype(BF16)

    natural(0)

    def project(owner, hi):
        rows = m256(owner)
        bias = wqp[hi, 192:208, 0:256].astype(F32)[0:1, :]
        part = (mm(h1[rows, :], wq[:, hi * 256:(hi + 1) * 256]) + bias).astype(BF16).astype(F32)
        q_s[hi, rows, :] = part[:, 0:64].astype(BF16)
        k_s[hi, rows, :] = part[:, 64:128].astype(BF16)
        v_s[hi, rows, :] = part[:, 128:192].astype(BF16)
        qkvt[hi, :, rows] = part.T[:192, :].astype(BF16)

    def near(t):
        base = chip + lax.div(t, 2) * (side - chip)
        return base + lax.rem(t, 2) * (chips - 1 - 2 * base)

    @pl.loop(0, chips)
    def _(t):
        src = near(t)

        @pl.when(t == 2)
        def _():
            wq_copy().start()
            wo_start(1, 2)
            w_start(1, 2, 3)

        @pl.when(t > 0)
        def _():
            h1_recv(t - 1, src).wait_recv()
            h1_pair(src, False).start()

        @pl.when(t == 1)
        def _():
            h1_copy(2).start()

        project(2 * src + core, 0)
        h1_pair(src, True).wait_recv()
        project(2 * src + 1 - core, 0)


    s_fac = attn_scale * LOG2E
    keep = lax.broadcasted_iota(jnp.int32, (256, 256), 0) <= lax.broadcasted_iota(jnp.int32, (256, 256), 1)

    def o_copy(hi, j):
        head = me + hi * (mate - me)
        return rc(o_own.at[hi, :, m256(j)], o_all.at[m64(head), m256(seq)], o_ss.at[hi, j], o_rs.at[seq, head], j)

    def fold(value, op):
        return op(value.reshape(32, 8, 256), axis=0)

    def attend(hi, j):
        cols = m256(j)
        q_t = qkvt[hi, 0:64, cols]
        base = 8 * (j % 2)
        m = jnp.full((8, 256), -1e30, F32)
        for kc in range(j + 1):
            s = mm(k_s[hi, m256(kc), :], q_t) * s_fac
            if kc == j:
                s = jnp.where(keep, s, -1e30)
            big[base + kc] = s
            m = jnp.maximum(m, fold(s, jnp.max))
        m = jnp.max(m, axis=0, keepdims=True)
        l = jnp.zeros((8, 256), F32)
        for kc in range(j + 1):
            l = l + fold(jnp.exp2(big[base + kc] - m), jnp.sum)
        lse_j = m + jnp.log2(jnp.sum(l, axis=0, keepdims=True))
        lse[hi, :, cols] = lse_j
        o = jnp.zeros((64, 256), F32)
        for kc in range(j + 1):
            p = jnp.exp2(big[base + kc] - lse_j).astype(BF16)
            o = o + mm(qkvt[hi, 128:192, m256(kc)], p)
        o = o.astype(BF16)
        o_own[hi, :, cols] = o

        @pl.when(me != j)
        def _():
            o_copy(hi, j).start()

        @pl.when(me == j)
        def _():
            o_all[m64(me + hi * (mate - me)), m256(seq)] = o

    @pl.loop(0, 2)
    def _(hi):
        @pl.when(hi == 1)
        def _():
            wq_copy().wait_recv()
            natural(1)

            @pl.loop(0, n_dev)
            def _(owner):
                project(owner, 1)

        for j in range(n_dev):
            attend(hi, j)
            if j == 4:
                @pl.when(hi == 1)
                def _():
                    w_wait(1)
                    w_start(4)
            if j == 2:
                @pl.when(hi == 1)
                def _():
                    wo_wait(1)
                    wo_start(3, 5)
            if j == 6:
                @pl.when(hi == 1)
                def _():
                    wo_wait(2, 3)
                    wo_start(4, 6)

    mate_copy(2).start()
    w_wait(2)
    w_start(5)
    w_wait(3)
    w_start(6, 7)
    wo_wait(0, 4, 5, 6)
    for n in range(n_dev):
        wo_all[n * 64:(n + 1) * 64, :] = wob[n, 0:64, :]
    for st in range(2):
        for n in range(n_dev):
            @pl.when(me != handler(n, st))
            def _():
                rc(o_own.at[0, :, m256(0)], o_all.at[m64(n), m256(st)], o_ss.at[0, 0], o_rs.at[st, n], PT).wait_recv()

    bias_o = vector(bo)
    gain2, shift2 = vector(g2), vector(s2)
    for r in range(4):
        rows = slice(r * 128, r * 128 + 128)
        attn = mm(o_all[:, rows], wo_all[...], 0, 0)
        x1_r = (x[rows, :].astype(F32) + attn + bias_o).astype(BF16)
        x1[rows, :] = x1_r
        x_hat, _ = norm_stats(x1_r.astype(F32))
        hh[rows, :] = (x_hat * gain2 + shift2).astype(BF16)
        if r % 2 == 1:
            mate_copy(r // 2).start()

    def mlp(n, rows):
        w2 = wp[n, 0:256, :]
        w1t = wp[n, 256:512, :]
        bias_u = wob[n, 64:80, 0:256].astype(F32)[0:1, :]
        z = (mm(hh[rows, :], w1t, 1, 1) + bias_u).astype(BF16).astype(F32)
        z2 = z * z
        th = jnp.tanh(GELU_A * (z + GELU_B * z2 * z))
        g = (0.5 * z * (1.0 + th)).astype(BF16)
        slope = 0.5 * (1.0 + th) + 0.5 * z * (1.0 - th * th) * (GELU_A * (1.0 + 3.0 * GELU_B * z2))
        dgl = mm(dyy[rows, :], w2, 1, 1).astype(BF16).astype(F32)
        dz = (dgl * slope).astype(BF16)
        ga[n, rows, :] = g
        dza[n, rows, :] = dz
        return dz, w1t

    acc[...] = jnp.zeros_like(acc)

    @pl.loop(0, n_dev)
    def _(i):
        t, other = lax.div(i, 2), lax.rem(i, 2)
        near_chip = chip + lax.rem(t, 2) * (side - chip)
        n = 2 * (near_chip + lax.div(t, 2) * (chips - 1 - 2 * near_chip)) + core + other * (1 - 2 * core)
        for step, at in ((0, 1), (6, 3), (7, 5), (8, 7)):
            @pl.when(i == at)
            def _():
                w_wait(step)

        @pl.when(i == 6)
        def _():
            w_wait(4, 5)
            w_start(8)

        for r in range(2):
            rows = slice(r * 256, r * 256 + 256)
            dz, w1t = mlp(n, rows)
            acc[rows, :] += mm(dz, w1t)

    vec[...] = jnp.zeros_like(vec)
    for r in range(4):
        rows = slice(r * 128, r * 128 + 128)
        dh2 = acc[rows, :].astype(BF16).astype(F32)
        x_hat, inv_std = norm_stats(x1[rows, :].astype(F32))
        dy_r = dy[rows, :].astype(F32)
        dx1_r = (dy_r + norm_back(dh2, x_hat, inv_std, gain2)).astype(BF16)
        dx1[rows, :] = dx1_r
        vec[2:3, :] += jnp.sum(dx1_r.astype(F32), axis=0, keepdims=True)
        vec[3:4, :] += jnp.sum(dh2 * x_hat, axis=0, keepdims=True)
        vec[4:5, :] += jnp.sum(dh2, axis=0, keepdims=True)
        vec[5:6, :] += jnp.sum(dy_r, axis=0, keepdims=True)

    def do_copy(n, st):
        target = handler(n, st)
        hi = 0 if target == n else 1
        return rc(do_send.at[m64(n), m256(st)], do_all.at[hi, :, m256(me)], do_ss.at[n, st], do_rs.at[hi, me], target)

    for r in range(2):
        rows = slice(r * 256, r * 256 + 256)
        do_send[rows, :] = mm(wo_all[rows, :], dx1[...], 1, 1).astype(BF16)
    for n in range(n_dev):
        for st in range(2):
            @pl.when(me != handler(n, st))
            def _():
                do_copy(n, st).start()

            @pl.when(me == handler(n, st))
            def _():
                do_all[0 if handler(n, st) == n else 1, :, m256(me)] = do_send[m64(n), m256(st)]

    def wo_pair_copy(slot):
        return rc(dwop.at[2 * slot + 1 - core], dwo_pr.at[slot], op_ss.at[slot], op_rs.at[slot], PT)

    def wo_copy(t):
        return rc(dwop.at[2 * t + core], dwo_rx.at[chip], ox_ss.at[t], ox_rs.at[chip], 2 * t + core)

    for n in range(n_dev):
        dwop[n] = mm(o_all[m64(n), :], dx1[...])
    for t in range(chips):
        wo_pair_copy(t).start()

    acc[...] = jnp.zeros_like(acc)

    @pl.loop(0, n_dev)
    def _(n):
        for r in range(2):
            rows = slice(r * 256, r * 256 + 256)
            acc[rows, :] += mm(ga[n, rows, :], wp[n, 0:256, :])

    y_out[...] = (x1[...].astype(F32) + acc[...] + vector(bd)).astype(BF16)

    def pair_copy(which):
        return rc(dwp.at[2 * which], prx.at[which], pr_ss.at[which], pr_rs.at[which], PT)

    def side_copy(step):
        rows = pl.ds(step * (G_ROWS // 3), G_ROWS // 3)
        return rc(dwp.at[1, rows], frx.at[rows], fr_ss.at[step], fr_rs.at[step], flank)

    def pair_add(which):
        pair_copy(which).wait_recv()
        dwp[2 * which + 1] += prx[which]

    for t in range(chips):
        wo_pair_copy(t).wait_recv()
        dwop[2 * t + core] += dwo_pr[t]

    wo_copy(side).start()

    def block(i):
        which, own = lax.div(i, 2), lax.rem(i, 2)
        return which, own, 2 * (side + which * (chip - side)) + (1 - core) + own * (2 * core - 1)

    @pl.loop(0, 4)
    def _(i):
        _, _, n = block(i)
        own_rows = slice(0, 512)
        dwp[i, 0:256, :] = mm(ga[n, own_rows, :], dyy[own_rows, :], 0, 0)
        dwp[i, 256:512, :] = mm(dza[n, own_rows, :], hh[own_rows, :], 0, 0)
        dwp[i, 512:528, 0:256] = jnp.broadcast_to(jnp.sum(dza[n, own_rows, :].astype(F32), axis=0, keepdims=True), (16, 256))
        dwp[i, 512:528, 256:512] = jnp.zeros((16, 256), F32)

    mate_copy(2).wait_recv()
    for r in range(2):
        mate_copy(r).wait_recv()
        rows = slice(512 + r * 256, 768 + r * 256)

        @pl.loop(0, 4)
        def _(i):
            which, own, n = block(i)
            mlp(n, rows)
            dwp[i, 0:256, :] += mm(ga[n, rows, :], dyy[rows, :], 0, 0)
            dwp[i, 256:512, :] += mm(dza[n, rows, :], hh[rows, :], 0, 0)
            dwp[i, 512:528, 0:256] += jnp.broadcast_to(jnp.sum(dza[n, rows, :].astype(F32), axis=0, keepdims=True), (16, 256))
            if r == 1:
                @pl.when(own == 0)
                def _():
                    pair_copy(which).start()

                @pl.when(i == 2)
                def _():
                    pair_add(0)
                    for step in range(3):
                        side_copy(step).start()

    pair_add(1)

    for j in range(n_dev):
        for hi in range(2):
            @pl.when(me != j)
            def _():
                rc(do_send.at[m64(0), m256(0)], do_all.at[hi, :, m256(j)], do_ss.at[0, 0], do_rs.at[hi, j], PT).wait_recv()
            do_t = do_all[hi, :, m256(j)].astype(F32)
            do_s[hi, m256(j), :] = do_t.T.astype(BF16)
            delta[hi, :, m256(j)] = jnp.sum(do_t * o_own[hi, :, m256(j)].astype(F32), axis=0, keepdims=True)
    for t in range(chips):
        @pl.when((chip != t) & (side != t))
        def _():
            wo_copy(t).start()
    dwq[...] = jnp.zeros_like(dwq)

    def dwq_copy():
        return rc(dwq.at[1], dwq_r, wq_ss.at[1], wq_rs.at[1], mate)

    def dh_pair_copy(kb):
        return rc(dh_send.at[kb], dh_pair.at[kb // 2], dhp_ss.at[kb // 2], dhp_rs.at[kb // 2], PT)

    def dh_copy(kb):
        return rc(dh_send.at[kb], dh_all.at[chip], dh_ss.at[kb // 2], dh_rs.at[chip], kb)

    def dh_finish(kb):
        @pl.when(core == kb % 2)
        def _():
            dh_pair_copy(kb).wait_recv()
            total = (dh_send[kb].astype(F32) + dh_pair[kb // 2].astype(F32)).astype(BF16)
            dh_send[kb] = total

            @pl.when(me != kb)
            def _():
                dh_copy(kb).start()

            @pl.when(me == kb)
            def _():
                dh_all[chip] = total

    @pl.loop(0, 2)
    def _(i):
        hi = 1 - i

        @pl.when(i == 1)
        def _():
            dwq_copy().start()

        for kb in range(n_dev):
            rows = m256(kb)
            k_b, v_b, kt_b = k_s[hi, rows, :], v_s[hi, rows, :], qkvt[hi, 64:128, rows]
            dk = jnp.zeros((256, 64), F32)
            dv = jnp.zeros((256, 64), F32)
            for qb in range(kb, n_dev):
                cols = m256(qb)
                p = jnp.exp2(mm(k_b, qkvt[hi, 0:64, cols]) * s_fac - lse[hi, :, cols])
                if qb == kb:
                    p = jnp.where(keep, p, 0.0)
                dp = mm(v_b, do_all[hi, :, cols]).astype(BF16).astype(F32)
                ds = (p * (dp - delta[hi, :, cols]) * attn_scale).astype(BF16)
                dv = dv + mm(p.astype(BF16), do_s[hi, cols, :])
                dk = dk + mm(ds, q_s[hi, cols, :])
                dq = mm(kt_b, ds)
                if kb == 0:
                    dqt[:, cols] = dq
                else:
                    dqt[:, cols] += dq
            dqkvt[hi, 0:64, rows] = dqt[:, rows].astype(BF16)
            dqkvt[hi, 64:192, rows] = jnp.concatenate([dk, dv], axis=1).T.astype(BF16)
            blk = dqkvt[hi, :, rows]
            dwq[hi, 0:192, :] += mm(blk, h1[rows, :])
            dwq[hi, 192:200, 0:192] += mm(jnp.ones((8, 256), BF16), blk, 1, 1)

            @pl.when(i == 1)
            def _():
                dh = mm(dqkvt[0, :, rows], wqp[0, 0:192, :], 0, 0) + mm(dqkvt[1, :, rows], wqp[1, 0:192, :], 0, 0)
                dh_send[kb] = dh.astype(BF16)

                @pl.when(core != kb % 2)
                def _():
                    dh_pair_copy(kb).start()

                if kb > 0:
                    dh_finish(kb - 1)


    dh_finish(n_dev - 1)

    for step in range(3):
        side_copy(step).wait_recv()
    dwd_out[...] = dwp[3, 0:256, :] + frx[0:256, :]
    dwu_out[...] = (dwp[3, 256:512, :] + frx[256:512, :]).T
    dbu_out[...] = dwp[3, 512:520, 0:256] + frx[512:520, 0:256]
    dwo_rx[chip] = dwop[me]
    for t in range(chips):
        @pl.when(chip != t)
        def _():
            rc(dwop.at[0], dwo_rx.at[t], ox_ss.at[0], ox_rs.at[t], PT).wait_recv()
    dwo_out[...] = dwo_rx[0] + dwo_rx[1] + dwo_rx[2] + dwo_rx[3]

    for t in range(chips):
        @pl.when(chip != t)
        def _():
            rc(dh_send.at[0], dh_all.at[t], dh_ss.at[0], dh_rs.at[t], PT).wait_recv()

    for r in range(4):
        rows = slice(r * 128, r * 128 + 128)
        half = slice((r % 2) * 128, (r % 2) * 128 + 128)
        first = (r // 2) * (chips // 2)
        dh1 = (dh_all[first, half, :].astype(F32) + dh_all[first + 1, half, :].astype(F32)).astype(BF16).astype(F32)
        x_hat, inv_std = norm_stats(x[rows, :].astype(F32))
        dx_out[rows, :] = (dx1[rows, :].astype(F32) + norm_back(dh1, x_hat, inv_std, gain1)).astype(BF16)
        vec[0:1, :] += jnp.sum(dh1 * x_hat, axis=0, keepdims=True)
        vec[1:2, :] += jnp.sum(dh1, axis=0, keepdims=True)

    def vec_copy(j):
        return rc(vec, vec_all.at[me], v_ss.at[j], v_rs.at[me], j)

    for j in range(n_dev):
        @pl.when(me != j)
        def _():
            vec_copy(j).start()
    vec_all[me] = vec[...]
    dwq_copy().wait_recv()
    dwqkv_out[...] = dwq[0] + dwq_r[...]
    for j in range(n_dev):
        @pl.when(me != j)
        def _():
            rc(vec, vec_all.at[j], v_ss.at[0], v_rs.at[j], PT).wait_recv()
    total = vec_all[0]
    for j in range(1, n_dev):
        total = total + vec_all[j]
    vec_out[...] = total

    wq_copy().wait_send()
    dwq_copy().wait_send()
    for t in range(chips):
        h1_pair(t, False).wait_send()

        @pl.when(chip != t)
        def _():
            wo_copy(t).wait_send()

        wo_pair_copy(t).wait_send()
    for step in range(9):
        w_copy(step).wait_send()
    for step in range(7):
        wo_all_copy(step).wait_send()
    for step in range(3):
        h1_copy(step).wait_send()
    for step in range(3):
        mate_copy(step).wait_send()
    for which in range(2):
        pair_copy(which).wait_send()
    for step in range(3):
        side_copy(step).wait_send()
    for j in range(n_dev):
        @pl.when(me != j)
        def _():
            vec_copy(j).wait_send()
            for hi in range(2):
                o_copy(hi, j).wait_send()

        for st in range(2):
            @pl.when(me != handler(j, st))
            def _():
                do_copy(j, st).wait_send()

        @pl.when(core != j % 2)
        def _():
            dh_pair_copy(j).wait_send()

        @pl.when((core == j % 2) & (me != j))
        def _():
            dh_copy(j).wait_send()


def finish_kernel(y, dx, vec, dwqkv, dwo, dwu, dbu, dwd, y_o, dx_o, v0, v1, dwqkv_o, dbqkv_o, dwo_o, v2, v3, v4, dwu_o, dbu_o, dwd_o, v5):
    y_o[...] = y[...]
    dx_o[...] = dx[...]
    for i, ref in enumerate((v0, v1, v2, v3, v4, v5)):
        ref[...] = vec[i:i + 1, :].reshape(ref.shape)
    dwqkv_o[...] = dwqkv[0:192, :]
    for c in range(3):
        dbqkv_o[c] = dwqkv[192:193, c * 64:(c + 1) * 64]
    dwo_o[...] = dwo[...]
    dwu_o[...] = dwu[...]
    dbu_o[...] = dbu[0:1, :].reshape(dbu_o.shape)
    dwd_o[...] = dwd[...]


def solution(mesh):
    n_dev = mesh.shape["tp"]

    def device_step(hidden, grad_out, ln1_gain, ln1_bias, w_qkv, b_qkv, w_out, b_out, ln2_gain, ln2_bias, w_up, b_up, w_down, b_down):
        batch, tokens, d = hidden.shape
        rows = batch * tokens
        head = w_qkv.shape[-1]
        seq = tokens * n_dev
        ff = w_up.shape[1]
        chips = n_dev // 2
        attn_scale = head ** -0.5
        sds = jax.ShapeDtypeStruct
        vm = pltpu.VMEM

        def dma(*shape):
            return pltpu.SemaphoreType.DMA(shape)

        vspec = pl.BlockSpec(memory_space=pltpu.VMEM)
        outs = pl.pallas_call(
            lambda *refs: layer_kernel(n_dev, attn_scale, *refs),
            out_shape=(sds((rows, d), BF16), sds((rows, d), BF16), sds((8, d), F32), sds((200, d), F32),
                       sds((head, d), F32), sds((d, ff), F32), sds((8, ff), F32), sds((ff, d), F32)),
            in_specs=[vspec] * 14,
            out_specs=tuple([vspec] * 8),
            scratch_shapes=[
                vm((2, tokens, d), BF16), vm((seq, d), BF16), vm((n_dev, WO_ROWS, d), BF16), vm((n_dev, 2 * ff, d), BF16),
                vm((2, 208, d), BF16), vm((d, 512), BF16),
                vm((2, seq, head), BF16), vm((2, seq, head), BF16), vm((2, seq, head), BF16), vm((2, 3 * head, seq), BF16),
                vm((16, 256, 256), F32), vm((2, 1, seq), F32), vm((2, head, seq), BF16), vm((n_dev * head, rows), BF16),
                vm((n_dev * head, d), BF16), vm((rows, d), BF16), vm((2 * rows, d), BF16), vm((2 * rows, d), BF16),
                vm((n_dev, 2 * rows, ff), BF16), vm((n_dev, 2 * rows, ff), BF16), vm((rows, d), F32), vm((rows, d), BF16),
                vm((n_dev * head, rows), BF16), vm((2, head, seq), BF16), vm((2, seq, head), BF16),
                vm((2, 1, seq), F32), vm((head, seq), F32), vm((2, 3 * head, seq), BF16),
                vm((n_dev, tokens, d), BF16), vm((chips, tokens, d), BF16), vm((chips, tokens, d), BF16),
                vm((2, 200, d), F32), vm((200, d), F32),
                vm((4, G_ROWS, d), F32), vm((2, G_ROWS, d), F32), vm((G_ROWS, d), F32),
                vm((n_dev, head, d), F32), vm((chips, head, d), F32), vm((chips, head, d), F32),
                vm((8, d), F32), vm((n_dev, 8, d), F32),
                dma(chips), dma(chips), dma(chips), dma(chips), dma(2), dma(2), dma(7), dma(7), dma(2, n_dev), dma(2, n_dev),
                dma(n_dev, 2), dma(2, n_dev), dma(chips), dma(chips), dma(chips), dma(chips),
                dma(9), dma(9), dma(3), dma(3), dma(2), dma(2), dma(3), dma(3), dma(chips), dma(chips), dma(chips), dma(chips), dma(n_dev), dma(n_dev),
            ],
            compiler_params=pltpu.CompilerParams(collective_id=0, has_side_effects=True, vmem_limit_bytes=67043328),
            name="layer",
        )(hidden.reshape(rows, d), grad_out.reshape(rows, d), ln1_gain, ln1_bias, b_out, ln2_gain, ln2_bias, b_down,
          w_qkv.transpose(1, 2, 3, 0).reshape(3 * head, d), b_qkv, w_out.reshape(head, d), w_up, b_up, w_down)
        v1d = sds((d,), F32)
        y, dx, v0, v1, dwqkv_t, dbqkv, dwo, v2, v3, v4, dwu, dbu, dwd, v5 = pl.pallas_call(
            finish_kernel,
            out_shape=(sds((rows, d), BF16), sds((rows, d), BF16), v1d, v1d, sds((3 * head, d), F32), sds((3, 1, head), F32),
                       sds((head, d), F32), v1d, v1d, v1d, sds((d, ff), F32), sds((ff,), F32), sds((ff, d), F32), v1d),
            in_specs=[vspec] * 8,
            out_specs=tuple([vspec] * 14),
            name="finish",
        )(*outs)
        return (y.reshape(hidden.shape), dx.reshape(hidden.shape), v0, v1, dwqkv_t.reshape(3, 1, head, d).transpose(3, 0, 1, 2),
                dbqkv, dwo.reshape(w_out.shape), v2, v3, v4, dwu, dbu, dwd, v5)

    act_spec = P("dp", "tp", None)
    vec_spec = P(None)
    group_vec = P("dp")
    in_specs = (act_spec, act_spec, vec_spec, vec_spec, P(None, None, "tp", None), P(None, "tp", None), P("tp", None, None), vec_spec, vec_spec, vec_spec, P(None, "tp"), P("tp"), P("tp", None), vec_spec)
    out_specs = (act_spec, act_spec, group_vec, group_vec, P("dp", None, "tp", None), P("dp", "tp", None), P(("dp", "tp"), None, None), group_vec, group_vec, group_vec, P("dp", "tp"), P(("dp", "tp")), P(("dp", "tp"), None), group_vec)
    return jax.shard_map(device_step, mesh=mesh, in_specs=in_specs, out_specs=out_specs, check_vma=False)
```

```python
import jax
import jax.numpy as jnp
from jax import lax
from jax.experimental import pallas as pl
from jax.experimental.pallas import tpu as pltpu
from jax.sharding import PartitionSpec as P

LN_EPS = 1e-5
MESH = pl.DeviceIdType.MESH
F32 = jnp.float32
BF16 = jnp.bfloat16
LOG2E = 1.4426950408889634
GELU_A = 0.7978845608028654
GELU_AB = GELU_A * 0.044715

TOK = 256
WIDTH = 512
HEAD = 64
HALF = 128
QKV = 192
SUB = 8
TAIL = 320
WQ_ROWS = 208
PACK = 16
THREE = 3
DW_ROWS = 200
SEQ = 2048
FOUR = 4
WO_ROWS = 80
G_ROWS = 528


def mm(lhs, rhs, lc=1, rc=0):
    return lax.dot_general(lhs, rhs, (((lc,), (rc,)), ((), ())), preferred_element_type=F32)


def norm_stats(value):
    centered = value - jnp.mean(value, axis=-1, keepdims=True)
    inv_std = lax.rsqrt(jnp.mean(centered * centered, axis=-1, keepdims=True) + LN_EPS)
    return centered * inv_std, inv_std


def norm_back(grad, x_hat, inv_std, gain):
    scaled = grad * gain
    return inv_std * (scaled - jnp.mean(scaled, axis=-1, keepdims=True) - x_hat * jnp.mean(scaled * x_hat, axis=-1, keepdims=True))


def vector(ref):
    return ref[...].astype(F32).reshape(1, -1)


def layer_kernel(n_dev, attn_scale,
                 x, dy, g1, s1, bo, g2, s2, bd, wqkv, bqkv, wo, wu, bu, wd,
                 y_out, dx_out, vec_out, dwqkv_out, dwo_out, dwu_out, dbu_out, dwd_out,
                 h1own, h1, wob, wp, wqp, wq, q_s, k_s, v_s, qkvt, big, lse, o_own, o_all, wo_all, x1, hh, dyy, ga, dza, acc, dx1,
                 do_send, do_all, do_s, delta, dqt, p_b, ds_b, dqkvt, wq_cat, dh_send, dh_pair, dh_all, dwq, dwq_r,
                 dwp, prx, frx, dwop, dwo_pr, dwo_rx, vec, vec_all,
                 hs_ss, hs_rs, hp_ss, hp_rs, wq_ss, wq_rs, wb_ss, wb_rs, o_ss, o_rs, do_ss, do_rs, dhp_ss, dhp_rs, dh_ss, dh_rs,
                 wp_ss, wp_rs, mt_ss, mt_rs, pr_ss, pr_rs, fr_ss, fr_rs, op_ss, op_rs, ox_ss, ox_rs, v_ss, v_rs):
    me = lax.axis_index("tp")
    chips = n_dev // 2
    chip, core = lax.div(me, 2), lax.rem(me, 2)
    seq = lax.div(chip, chips // 2)
    mate = 2 * (chips - 1 - chip) + core
    side = chip + 1 - 2 * lax.rem(chip, 2)
    flank, across = 2 * side + core, 2 * (chips - 1 - side) + core

    def dev(shift, other):
        return 2 * lax.rem(chip + shift + chips, chips) + (1 - core if other else core)

    PT = dev(0, True)

    def handler(n, st):
        return n if (n // 2) // (chips // 2) == st else 2 * (chips - 1 - n // 2) + n % 2

    def rc(src, dst, ssem, rsem, target):
        return pltpu.make_async_remote_copy(src_ref=src, dst_ref=dst, send_sem=ssem, recv_sem=rsem,
                                            device_id={"tp": target}, device_id_type=MESH)

    def m256(i):
        return pl.ds(i * TOK, TOK) if isinstance(i, int) else pl.ds(pl.multiple_of(i * TOK, TOK), TOK)

    def m64(i):
        return pl.ds(i * HEAD, HEAD) if isinstance(i, int) else pl.ds(pl.multiple_of(i * HEAD, HEAD), HEAD)
    barrier = pltpu.get_barrier_semaphore()
    for i in range(n_dev):
        @pl.when(me != i)
        def _():
            pl.semaphore_signal(barrier, inc=1, device_id={"tp": i}, device_id_type=MESH)

    gain1, shift1 = vector(g1), vector(s1)
    for b in range(2):
        for r in range(2):
            rows = slice(b * TOK + r * HALF, b * TOK + r * HALF + HALF)
            x_hat, _ = norm_stats(x[rows, :].astype(F32))
            h1own[b, r * HALF:r * HALF + HALF, :] = (x_hat * gain1 + shift1).astype(BF16)
    h1[m256(me), :] = h1own[seq]
    wqp[0, 0:QKV, :] = wqkv[...]
    bq_row = jnp.concatenate([bqkv[c].astype(F32) for c in range(THREE)] + [jnp.zeros((1, TAIL), F32)], axis=1)
    wqp[0, QKV:WQ_ROWS, :] = jnp.broadcast_to(bq_row, (PACK, WIDTH)).astype(BF16)

    def h1_copy(step):
        src, row, target = ((h1own.at[1 - seq], me, mate), (h1own.at[seq], me, flank), (h1.at[m256(mate), :], mate, flank))[step]
        return rc(src, h1.at[m256(row), :], hs_ss.at[step], hs_rs.at[step], target)

    def h1_recv(step, src):
        return rc(h1own.at[0], h1.at[m256(2 * src + core), :], hs_ss.at[0], hs_rs.at[step], PT)

    def h1_pair(src, received):
        rows = m256(2 * src + (1 - core if received else core))
        return rc(h1.at[rows, :], h1.at[rows, :], hp_ss.at[src], hp_rs.at[src], PT)

    def wq_copy():
        return rc(wqp.at[0], wqp.at[1], wq_ss.at[0], wq_rs.at[0], mate)
    pl.semaphore_wait(barrier, n_dev - 1)
    h1_copy(0).start()
    h1_copy(1).start()
    h1_pair(chip, False).start()
    wob[me, 0:HEAD, :] = wo[...]
    wob[me, HEAD:80, 0:TOK] = jnp.broadcast_to(vector(bu), (PACK, TOK)).astype(BF16)
    wob[me, HEAD:80, TOK:WIDTH] = jnp.zeros((PACK, TOK), BF16)
    wp[me, 0:TOK, :] = wd[...]
    wp[me, TOK:WIDTH, :] = wu[...].astype(F32).T.astype(BF16)
    dyy[0:WIDTH, :] = dy[...]

    def twin(d):
        return d + 1 - 2 * core

    w_plan = ((me, PT, PT, 0, WIDTH), (me, mate, mate, 0, TOK), (me, mate, mate, TOK, TOK), (me, flank, flank, 0, WIDTH),
              (mate, flank, across, 0, TOK), (mate, flank, across, TOK, TOK),
              (flank, PT, twin(flank), 0, WIDTH), (mate, PT, twin(mate), 0, WIDTH), (across, PT, twin(across), 0, WIDTH))

    def w_copy(step, received=False):
        own, target, got, off, size = w_plan[step]
        v = wp.at[got if received else own, pl.ds(off, size), :]
        return rc(v, v, wp_ss.at[step], wp_rs.at[step], target)

    def w_wait(*steps):
        for step in steps:
            w_copy(step, True).wait_recv()

    def w_start(*steps):
        for step in steps:
            w_copy(step).start()

    o_plan = ((me, PT, PT), (me, mate, mate), (me, flank, flank), (mate, flank, across),
              (flank, PT, twin(flank)), (mate, PT, twin(mate)), (across, PT, twin(across)))

    def wo_all_copy(step, received=False):
        own, target, got = o_plan[step]
        v = wob.at[got if received else own]
        return rc(v, v, wb_ss.at[step], wb_rs.at[step], target)

    def wo_wait(*steps):
        for step in steps:
            wo_all_copy(step, True).wait_recv()

    def wo_start(*steps):
        for step in steps:
            wo_all_copy(step).start()

    wo_start(0)

    def mate_copy(step):
        src, dst = ((hh.at[0:TOK], hh.at[WIDTH:768]), (hh.at[TOK:WIDTH], hh.at[768:1024]), (dyy.at[0:WIDTH], dyy.at[WIDTH:1024]))[step]
        return rc(src, dst, mt_ss.at[step], mt_rs.at[step], mate)

    w_start(0)

    def natural(hi):
        full = jnp.concatenate([wqp[hi, 0:QKV, :].astype(F32), jnp.zeros((HEAD, WIDTH), F32)], axis=0)
        wq[:, hi * TOK:(hi + 1) * TOK] = full.T.astype(BF16)

    natural(0)

    def project(owner, hi):
        rows = m256(owner)
        bias = wqp[hi, QKV:WQ_ROWS, 0:TOK].astype(F32)[0:1, :]
        part = (mm(h1[rows, :], wq[:, hi * TOK:(hi + 1) * TOK]) + bias).astype(BF16).astype(F32)
        q_s[hi, rows, :] = part[:, 0:HEAD].astype(BF16)
        k_s[hi, rows, :] = part[:, HEAD:HALF].astype(BF16)
        v_s[hi, rows, :] = part[:, HALF:QKV].astype(BF16)
        qkvt[hi, :, rows] = part.T[:QKV, :].astype(BF16)

    def near(t):
        base = chip + lax.div(t, 2) * (side - chip)
        return base + lax.rem(t, 2) * (chips - 1 - 2 * base)
    @pl.loop(0, chips)
    def _(t):
        src = near(t)

        @pl.when(t == 2)
        def _():
            wq_copy().start()
            wo_start(1, 2)
            w_start(1, 2, THREE)

        @pl.when(t > 0)
        def _():
            h1_recv(t - 1, src).wait_recv()
            h1_pair(src, False).start()

        @pl.when(t == 1)
        def _():
            h1_copy(2).start()

        project(2 * src + core, 0)
        h1_pair(src, True).wait_recv()
        project(2 * src + 1 - core, 0)


    s_fac = attn_scale * LOG2E
    keep = lax.broadcasted_iota(jnp.int32, (TOK, TOK), 0) <= lax.broadcasted_iota(jnp.int32, (TOK, TOK), 1)

    def o_copy(hi, j):
        head = me + hi * (mate - me)
        return rc(o_own.at[hi, :, m256(j)], o_all.at[m64(head), m256(seq)], o_ss.at[hi, j], o_rs.at[seq, head], j)

    def fold(value, op):
        return op(value.reshape(32, SUB, TOK), axis=0)

    def attend(hi, j):
        cols = m256(j)
        q_t = qkvt[hi, 0:HEAD, cols]
        base = SUB * (j % 2)
        m = jnp.full((SUB, TOK), -1e30, F32)
        for kc in range(j + 1):
            s = mm(k_s[hi, m256(kc), :], q_t) * s_fac
            if kc == j:
                s = jnp.where(keep, s, -1e30)
            big[base + kc] = s
            m = jnp.maximum(m, fold(s, jnp.max))
        m = jnp.max(m, axis=0, keepdims=True)
        l = jnp.zeros((SUB, TOK), F32)
        for kc in range(j + 1):
            l = l + fold(jnp.exp2(big[base + kc] - m), jnp.sum)
        lse_j = m + jnp.log2(jnp.sum(l, axis=0, keepdims=True))
        lse[hi, :, cols] = lse_j
        o = jnp.zeros((HEAD, TOK), F32)
        for kc in range(j + 1):
            p = jnp.exp2(big[base + kc] - lse_j).astype(BF16)
            o = o + mm(qkvt[hi, HALF:QKV, m256(kc)], p)
        o = o.astype(BF16)
        o_own[hi, :, cols] = o

        @pl.when(me != j)
        def _():
            o_copy(hi, j).start()

        @pl.when(me == j)
        def _():
            o_all[m64(me + hi * (mate - me)), m256(seq)] = o
    @pl.loop(0, 2)
    def _(hi):
        @pl.when(hi == 1)
        def _():
            wq_copy().wait_recv()
            natural(1)

            @pl.loop(0, n_dev)
            def _(owner):
                project(owner, 1)

        for j in range(n_dev):
            attend(hi, j)
            if j == 2:
                @pl.when(hi == 1)
                def _():
                    wo_wait(1)
                    wo_start(THREE, 5)
            if j == 6:
                @pl.when(hi == 1)
                def _():
                    wo_wait(2, THREE)
                    wo_start(FOUR, 6)
    mate_copy(2).start()
    w_wait(1, 2)
    w_start(FOUR, 5)
    w_wait(THREE)
    w_start(6, 7)
    wo_wait(0, FOUR, 5, 6)
    for n in range(n_dev):
        wo_all[n * HEAD:(n + 1) * HEAD, :] = wob[n, 0:HEAD, :]
    for st in range(2):
        for n in range(n_dev):
            @pl.when(me != handler(n, st))
            def _():
                rc(o_own.at[0, :, m256(0)], o_all.at[m64(n), m256(st)], o_ss.at[0, 0], o_rs.at[st, n], PT).wait_recv()

    bias_o = vector(bo)
    gain2, shift2 = vector(g2), vector(s2)
    for r in range(FOUR):
        rows = slice(r * HALF, r * HALF + HALF)
        attn = mm(o_all[:, rows], wo_all[...], 0, 0)
        x1_r = (x[rows, :].astype(F32) + attn + bias_o).astype(BF16)
        x1[rows, :] = x1_r
        x_hat, _ = norm_stats(x1_r.astype(F32))
        hh[rows, :] = (x_hat * gain2 + shift2).astype(BF16)
        if r % 2 == 1:
            mate_copy(r // 2).start()

    def mlp(n, rows):
        w2 = wp[n, 0:TOK, :]
        w1t = wp[n, TOK:WIDTH, :]
        bias_u = wob[n, HEAD:80, 0:TOK].astype(F32)[0:1, :]
        z = (mm(hh[rows, :], w1t, 1, 1) + bias_u).astype(BF16).astype(F32)
        z2 = z * z
        h = 0.5 * jnp.tanh(z * (GELU_A + GELU_AB * z2)) + 0.5
        g = z * h
        slope = h + g * ((1.0 - h) * (2.0 * GELU_A + 6.0 * GELU_AB * z2))
        dgl = mm(dyy[rows, :], w2, 1, 1).astype(BF16).astype(F32)
        dz = (dgl * slope).astype(BF16)
        ga[n, rows, :] = g.astype(BF16)
        dza[n, rows, :] = dz
        return dz, w1t
    acc[...] = jnp.zeros_like(acc)

    @pl.loop(0, n_dev)
    def _(i):
        t, other = lax.div(i, 2), lax.rem(i, 2)
        near_chip = chip + lax.rem(t, 2) * (side - chip)
        n = 2 * (near_chip + lax.div(t, 2) * (chips - 1 - 2 * near_chip)) + core + other * (1 - 2 * core)
        for step, at in ((0, 1), (6, THREE), (7, 5), (SUB, 7)):
            @pl.when(i == at)
            def _():
                w_wait(step)

        @pl.when(i == 6)
        def _():
            w_wait(FOUR, 5)
            w_start(SUB)

        for r in range(2):
            rows = slice(r * TOK, r * TOK + TOK)
            dz, w1t = mlp(n, rows)
            acc[rows, :] += mm(dz, w1t)
    vec[...] = jnp.zeros_like(vec)
    for r in range(FOUR):
        rows = slice(r * HALF, r * HALF + HALF)
        dh2 = acc[rows, :].astype(BF16).astype(F32)
        x_hat, inv_std = norm_stats(x1[rows, :].astype(F32))
        dy_r = dy[rows, :].astype(F32)
        dx1_r = (dy_r + norm_back(dh2, x_hat, inv_std, gain2)).astype(BF16)
        dx1[rows, :] = dx1_r
        vec[2:THREE, :] += jnp.sum(dx1_r.astype(F32), axis=0, keepdims=True)
        vec[THREE:FOUR, :] += jnp.sum(dh2 * x_hat, axis=0, keepdims=True)
        vec[FOUR:5, :] += jnp.sum(dh2, axis=0, keepdims=True)
        vec[5:6, :] += jnp.sum(dy_r, axis=0, keepdims=True)

    def do_copy(n, st):
        target = handler(n, st)
        hi = 0 if target == n else 1
        return rc(do_send.at[m64(n), m256(st)], do_all.at[hi, :, m256(me)], do_ss.at[n, st], do_rs.at[hi, me], target)

    for r in range(2):
        rows = slice(r * TOK, r * TOK + TOK)
        do_send[rows, :] = mm(wo_all[rows, :], dx1[...], 1, 1).astype(BF16)
    for n in range(n_dev):
        for st in range(2):
            @pl.when(me != handler(n, st))
            def _():
                do_copy(n, st).start()

            @pl.when(me == handler(n, st))
            def _():
                do_all[0 if handler(n, st) == n else 1, :, m256(me)] = do_send[m64(n), m256(st)]

    def wo_pair_copy(slot):
        return rc(dwop.at[2 * slot + 1 - core], dwo_pr.at[slot], op_ss.at[slot], op_rs.at[slot], PT)

    def wo_copy(t):
        return rc(dwop.at[2 * t + core], dwo_rx.at[chip], ox_ss.at[t], ox_rs.at[chip], 2 * t + core)
    for n in range(n_dev):
        dwop[n] = mm(o_all[m64(n), :], dx1[...])
    for t in range(chips):
        wo_pair_copy(t).start()

    def pair_copy(which):
        return rc(dwp.at[2 * which], prx.at[which], pr_ss.at[which], pr_rs.at[which], PT)

    def side_copy(step):
        rows = pl.ds(step * (G_ROWS // THREE), G_ROWS // THREE)
        return rc(dwp.at[1, rows], frx.at[rows], fr_ss.at[step], fr_rs.at[step], flank)

    def pair_add(which):
        pair_copy(which).wait_recv()
        dwp[2 * which + 1] += prx[which]

    for t in range(chips):
        wo_pair_copy(t).wait_recv()
        dwop[2 * t + core] += dwo_pr[t]

    wo_copy(side).start()

    def block(i):
        which, own = lax.div(i, 2), lax.rem(i, 2)
        return which, own, 2 * (side + which * (chip - side)) + (1 - core) + own * (2 * core - 1)
    @pl.loop(0, FOUR)
    def _(i):
        _, _, n = block(i)
        own_rows = slice(0, WIDTH)
        dwp[i, 0:TOK, :] = mm(ga[n, own_rows, :], dyy[own_rows, :], 0, 0)
        dwp[i, TOK:WIDTH, :] = mm(dza[n, own_rows, :], hh[own_rows, :], 0, 0)
        dwp[i, WIDTH:528, 0:TOK] = jnp.broadcast_to(jnp.sum(dza[n, own_rows, :].astype(F32), axis=0, keepdims=True), (PACK, TOK))
        dwp[i, WIDTH:528, TOK:WIDTH] = jnp.zeros((PACK, TOK), F32)
    mate_copy(2).wait_recv()
    for r in range(2):
        mate_copy(r).wait_recv()
        rows = slice(WIDTH + r * TOK, 768 + r * TOK)
        @pl.loop(0, FOUR)
        def _(i):
            which, own, n = block(i)
            mlp(n, rows)
            dwp[i, 0:TOK, :] += mm(ga[n, rows, :], dyy[rows, :], 0, 0)
            dwp[i, TOK:WIDTH, :] += mm(dza[n, rows, :], hh[rows, :], 0, 0)
            dwp[i, WIDTH:528, 0:TOK] += jnp.broadcast_to(jnp.sum(dza[n, rows, :].astype(F32), axis=0, keepdims=True), (PACK, TOK))
            if r == 1:
                @pl.when(own == 0)
                def _():
                    pair_copy(which).start()

                @pl.when(i == 2)
                def _():
                    pair_add(0)
                    for step in range(THREE):
                        side_copy(step).start()

    pair_add(1)

    for j in range(n_dev):
        for hi in range(2):
            @pl.when(me != j)
            def _():
                rc(do_send.at[m64(0), m256(0)], do_all.at[hi, :, m256(j)], do_ss.at[0, 0], do_rs.at[hi, j], PT).wait_recv()
            do_t = do_all[hi, :, m256(j)].astype(F32)
            do_s[hi, m256(j), :] = do_t.T.astype(BF16)
            delta[hi, :, m256(j)] = jnp.sum(do_t * o_own[hi, :, m256(j)].astype(F32), axis=0, keepdims=True)
    for t in range(chips):
        @pl.when((chip != t) & (side != t))
        def _():
            wo_copy(t).start()
    dwq[...] = jnp.zeros_like(dwq)
    for hi in range(2):
        wq_cat[hi * QKV:(hi + 1) * QKV, :] = wqp[hi, 0:QKV, :]

    def dwq_copy():
        return rc(dwq.at[1], dwq_r, wq_ss.at[1], wq_rs.at[1], mate)

    def dh_pair_copy(kb):
        return rc(dh_send.at[kb], dh_pair.at[kb // 2], dhp_ss.at[kb // 2], dhp_rs.at[kb // 2], PT)

    def dh_copy(kb):
        return rc(dh_send.at[kb], dh_all.at[chip], dh_ss.at[kb // 2], dh_rs.at[chip], kb)

    def dh_finish(kb):
        @pl.when(core == kb % 2)
        def _():
            dh_pair_copy(kb).wait_recv()
            total = (dh_send[kb].astype(F32) + dh_pair[kb // 2].astype(F32)).astype(BF16)
            dh_send[kb] = total

            @pl.when(me != kb)
            def _():
                dh_copy(kb).start()

            @pl.when(me == kb)
            def _():
                dh_all[chip] = total
    @pl.loop(0, 2)
    def _(i):
        hi = 1 - i
        base = pl.multiple_of(QKV * hi, HEAD)

        @pl.when(i == 1)
        def _():
            dwq_copy().start()

        for kb in range(n_dev):
            rows = m256(kb)
            late = slice(kb * TOK, n_dev * TOK)
            for qb in range(kb, n_dev):
                cols = m256(qb)
                for c in range(2):
                    part = slice(c * HALF, c * HALF + HALF)
                    keys = slice(kb * TOK + c * HALF, kb * TOK + c * HALF + HALF)
                    p = jnp.exp2(mm(k_s[hi, keys, :], qkvt[hi, 0:HEAD, cols]) * s_fac - lse[hi, :, cols])
                    if qb == kb:
                        p = jnp.where(keep[part], p, 0.0)
                    dp = mm(v_s[hi, keys, :], do_all[hi, :, cols]).astype(BF16).astype(F32)
                    p_b[kb % 2, part, cols] = p.astype(BF16)
                    ds_b[kb % 2, part, cols] = (p * (dp - delta[hi, :, cols])).astype(BF16)
            dv = mm(p_b[kb % 2, :, late], do_s[hi, late, :])
            dk = mm(ds_b[kb % 2, :, late], q_s[hi, late, :]) * attn_scale
            dq = mm(qkvt[hi, HEAD:HALF, rows], ds_b[kb % 2, :, late])
            if kb == 0:
                dqt[...] = dq
            else:
                dqt[:, late] += dq
            dqkvt[pl.ds(base, HEAD), rows] = (dqt[:, rows] * attn_scale).astype(BF16)
            dqkvt[pl.ds(base + HEAD, HALF), rows] = jnp.concatenate([dk, dv], axis=1).T.astype(BF16)

            @pl.when(i == 1)
            def _():
                dh = mm(dqkvt[:, rows], wq_cat[...], 0, 0)
                dh_send[kb] = dh.astype(BF16)

                @pl.when(core != kb % 2)
                def _():
                    dh_pair_copy(kb).start()

                if kb > 0:
                    dh_finish(kb - 1)


        mine = dqkvt[pl.ds(base, QKV), :]
        dwq[hi, 0:QKV, :] = mm(mine, h1[...])
        dwq[hi, QKV:DW_ROWS, 0:QKV] = mm(jnp.ones((SUB, SEQ), BF16), mine, 1, 1)

    dh_finish(n_dev - 1)

    for step in range(THREE):
        side_copy(step).wait_recv()
    dwd_out[...] = dwp[THREE, 0:TOK, :] + frx[0:TOK, :]
    dwu_out[...] = (dwp[THREE, TOK:WIDTH, :] + frx[TOK:WIDTH, :]).T
    dbu_out[...] = dwp[THREE, WIDTH:520, 0:TOK] + frx[WIDTH:520, 0:TOK]
    dwo_rx[chip] = dwop[me]
    for t in range(chips):
        @pl.when(chip != t)
        def _():
            rc(dwop.at[0], dwo_rx.at[t], ox_ss.at[0], ox_rs.at[t], PT).wait_recv()
    dwo_out[...] = dwo_rx[0] + dwo_rx[1] + dwo_rx[2] + dwo_rx[THREE]

    acc[...] = jnp.zeros_like(acc)

    @pl.loop(0, n_dev)
    def _(n):
        for r in range(2):
            rows = slice(r * TOK, r * TOK + TOK)
            acc[rows, :] += mm(ga[n, rows, :], wp[n, 0:TOK, :])

    y_out[...] = (x1[...].astype(F32) + acc[...] + vector(bd)).astype(BF16)

    for t in range(chips):
        @pl.when(chip != t)
        def _():
            rc(dh_send.at[0], dh_all.at[t], dh_ss.at[0], dh_rs.at[t], PT).wait_recv()
    for r in range(FOUR):
        rows = slice(r * HALF, r * HALF + HALF)
        half = slice((r % 2) * HALF, (r % 2) * HALF + HALF)
        first = (r // 2) * (chips // 2)
        dh1 = (dh_all[first, half, :].astype(F32) + dh_all[first + 1, half, :].astype(F32)).astype(BF16).astype(F32)
        x_hat, inv_std = norm_stats(x[rows, :].astype(F32))
        dx_out[rows, :] = (dx1[rows, :].astype(F32) + norm_back(dh1, x_hat, inv_std, gain1)).astype(BF16)
        vec[0:1, :] += jnp.sum(dh1 * x_hat, axis=0, keepdims=True)
        vec[1:2, :] += jnp.sum(dh1, axis=0, keepdims=True)

    def vec_copy(j):
        return rc(vec, vec_all.at[me], v_ss.at[j], v_rs.at[me], j)
    for j in range(n_dev):
        @pl.when(me != j)
        def _():
            vec_copy(j).start()
    vec_all[me] = vec[...]
    dwq_copy().wait_recv()
    dwqkv_out[...] = dwq[0] + dwq_r[...]
    for j in range(n_dev):
        @pl.when(me != j)
        def _():
            rc(vec, vec_all.at[j], v_ss.at[0], v_rs.at[j], PT).wait_recv()
    total = vec_all[0]
    for j in range(1, n_dev):
        total = total + vec_all[j]
    vec_out[...] = total

    wq_copy().wait_send()
    dwq_copy().wait_send()
    for t in range(chips):
        h1_pair(t, False).wait_send()

        @pl.when(chip != t)
        def _():
            wo_copy(t).wait_send()

        wo_pair_copy(t).wait_send()
    for step in range(9):
        w_copy(step).wait_send()
    for step in range(7):
        wo_all_copy(step).wait_send()
    for step in range(THREE):
        h1_copy(step).wait_send()
    for step in range(THREE):
        mate_copy(step).wait_send()
    for which in range(2):
        pair_copy(which).wait_send()
    for step in range(THREE):
        side_copy(step).wait_send()
    for j in range(n_dev):
        @pl.when(me != j)
        def _():
            vec_copy(j).wait_send()
            for hi in range(2):
                o_copy(hi, j).wait_send()

        for st in range(2):
            @pl.when(me != handler(j, st))
            def _():
                do_copy(j, st).wait_send()

        @pl.when(core != j % 2)
        def _():
            dh_pair_copy(j).wait_send()

        @pl.when((core == j % 2) & (me != j))
        def _():
            dh_copy(j).wait_send()


def finish_kernel(y, dx, vec, dwqkv, dwo, dwu, dbu, dwd, y_o, dx_o, v0, v1, dwqkv_o, dbqkv_o, dwo_o, v2, v3, v4, dwu_o, dbu_o, dwd_o, v5):
    y_o[...] = y[...]
    dx_o[...] = dx[...]
    for i, ref in enumerate((v0, v1, v2, v3, v4, v5)):
        ref[...] = vec[i:i + 1, :].reshape(ref.shape)
    dwqkv_o[...] = dwqkv[0:QKV, :]
    for c in range(THREE):
        dbqkv_o[c] = dwqkv[QKV:193, c * HEAD:(c + 1) * HEAD]
    dwo_o[...] = dwo[...]
    dwu_o[...] = dwu[...]
    dbu_o[...] = dbu[0:1, :].reshape(dbu_o.shape)
    dwd_o[...] = dwd[...]


def solution(mesh):
    n_dev = mesh.shape["tp"]

    def device_step(hidden, grad_out, ln1_gain, ln1_bias, w_qkv, b_qkv, w_out, b_out, ln2_gain, ln2_bias, w_up, b_up, w_down, b_down):
        batch, tokens, d = hidden.shape
        rows = batch * tokens
        head = w_qkv.shape[-1]
        seq = tokens * n_dev
        ff = w_up.shape[1]
        chips = n_dev // 2
        attn_scale = head ** -0.5
        sds = jax.ShapeDtypeStruct
        vm = pltpu.VMEM

        def dma(*shape):
            return pltpu.SemaphoreType.DMA(shape)

        vspec = pl.BlockSpec(memory_space=pltpu.VMEM)
        outs = pl.pallas_call(
            lambda *refs: layer_kernel(n_dev, attn_scale, *refs),
            out_shape=(sds((rows, d), BF16), sds((rows, d), BF16), sds((SUB, d), F32), sds((DW_ROWS, d), F32),
                       sds((head, d), F32), sds((d, ff), F32), sds((SUB, ff), F32), sds((ff, d), F32)),
            in_specs=[vspec] * 14,
            out_specs=tuple([vspec] * SUB),
            scratch_shapes=[
                vm((2, tokens, d), BF16), vm((seq, d), BF16), vm((n_dev, WO_ROWS, d), BF16), vm((n_dev, 2 * ff, d), BF16),
                vm((2, WQ_ROWS, d), BF16), vm((d, WIDTH), BF16),
                vm((2, seq, head), BF16), vm((2, seq, head), BF16), vm((2, seq, head), BF16), vm((2, THREE * head, seq), BF16),
                vm((PACK, TOK, TOK), F32), vm((2, 1, seq), F32), vm((2, head, seq), BF16), vm((n_dev * head, rows), BF16),
                vm((n_dev * head, d), BF16), vm((rows, d), BF16), vm((2 * rows, d), BF16), vm((2 * rows, d), BF16),
                vm((n_dev, 2 * rows, ff), BF16), vm((n_dev, 2 * rows, ff), BF16), vm((rows, d), F32), vm((rows, d), BF16),
                vm((n_dev * head, rows), BF16), vm((2, head, seq), BF16), vm((2, seq, head), BF16),
                vm((2, 1, seq), F32), vm((head, seq), F32), vm((2, TOK, seq), BF16), vm((2, TOK, seq), BF16), vm((6 * head, seq), BF16), vm((6 * head, d), BF16),
                vm((n_dev, tokens, d), BF16), vm((chips, tokens, d), BF16), vm((chips, tokens, d), BF16),
                vm((2, DW_ROWS, d), F32), vm((DW_ROWS, d), F32),
                vm((FOUR, G_ROWS, d), F32), vm((2, G_ROWS, d), F32), vm((G_ROWS, d), F32),
                vm((n_dev, head, d), F32), vm((chips, head, d), F32), vm((chips, head, d), F32),
                vm((SUB, d), F32), vm((n_dev, SUB, d), F32),
                dma(chips), dma(chips), dma(chips), dma(chips), dma(2), dma(2), dma(7), dma(7), dma(2, n_dev), dma(2, n_dev),
                dma(n_dev, 2), dma(2, n_dev), dma(chips), dma(chips), dma(chips), dma(chips),
                dma(9), dma(9), dma(THREE), dma(THREE), dma(2), dma(2), dma(THREE), dma(THREE), dma(chips), dma(chips), dma(chips), dma(chips), dma(n_dev), dma(n_dev),
            ],
            compiler_params=pltpu.CompilerParams(collective_id=0, has_side_effects=True, vmem_limit_bytes=67043328),
            name="layer",
        )(hidden.reshape(rows, d), grad_out.reshape(rows, d), ln1_gain, ln1_bias, b_out, ln2_gain, ln2_bias, b_down,
          w_qkv.transpose(1, 2, THREE, 0).reshape(THREE * head, d), b_qkv, w_out.reshape(head, d), w_up, b_up, w_down)
        v1d = sds((d,), F32)
        y, dx, v0, v1, dwqkv_t, dbqkv, dwo, v2, v3, v4, dwu, dbu, dwd, v5 = pl.pallas_call(
            finish_kernel,
            out_shape=(sds((rows, d), BF16), sds((rows, d), BF16), v1d, v1d, sds((THREE * head, d), F32), sds((THREE, 1, head), F32),
                       sds((head, d), F32), v1d, v1d, v1d, sds((d, ff), F32), sds((ff,), F32), sds((ff, d), F32), v1d),
            in_specs=[vspec] * SUB,
            out_specs=tuple([vspec] * 14),
            name="finish",
        )(*outs)
        return (y.reshape(hidden.shape), dx.reshape(hidden.shape), v0, v1, dwqkv_t.reshape(THREE, 1, head, d).transpose(THREE, 0, 1, 2),
                dbqkv, dwo.reshape(w_out.shape), v2, v3, v4, dwu, dbu, dwd, v5)

    act_spec = P("dp", "tp", None)
    vec_spec = P(None)
    group_vec = P("dp")
    in_specs = (act_spec, act_spec, vec_spec, vec_spec, P(None, None, "tp", None), P(None, "tp", None), P("tp", None, None), vec_spec, vec_spec, vec_spec, P(None, "tp"), P("tp"), P("tp", None), vec_spec)
    out_specs = (act_spec, act_spec, group_vec, group_vec, P("dp", None, "tp", None), P("dp", "tp", None), P(("dp", "tp"), None, None), group_vec, group_vec, group_vec, P("dp", "tp"), P(("dp", "tp")), P(("dp", "tp"), None), group_vec)
    return jax.shard_map(device_step, mesh=mesh, in_specs=in_specs, out_specs=out_specs, check_vma=False)
```

```python
import jax
import jax.numpy as jnp
from jax import lax
from jax.experimental import pallas as pl
from jax.experimental.pallas import tpu as pltpu
from jax.sharding import PartitionSpec as P

LN_EPS = 1e-5
MESH = pl.DeviceIdType.MESH
F32 = jnp.float32
BF16 = jnp.bfloat16
LOG2E = 1.4426950408889634
GELU_A = 0.7978845608028654
GELU_AB = GELU_A * 0.044715

TOK = 256
WIDTH = 512
HEAD = 64
HALF = 128
QKV = 192
SUB = 8
TAIL = 320
WQ_ROWS = 208
PACK = 16
THREE = 3
DW_ROWS = 200
SEQ = 2048
FOUR = 4
WO_ROWS = 80
G_ROWS = 528


def mm(lhs, rhs, lc=1, rc=0):
    return lax.dot_general(lhs, rhs, (((lc,), (rc,)), ((), ())), preferred_element_type=F32)


def norm_stats(value):
    centered = value - jnp.mean(value, axis=-1, keepdims=True)
    inv_std = lax.rsqrt(jnp.mean(centered * centered, axis=-1, keepdims=True) + LN_EPS)
    return centered * inv_std, inv_std


def norm_back(grad, x_hat, inv_std, gain):
    scaled = grad * gain
    return inv_std * (scaled - jnp.mean(scaled, axis=-1, keepdims=True) - x_hat * jnp.mean(scaled * x_hat, axis=-1, keepdims=True))


def vector(ref):
    return ref[...].astype(F32).reshape(1, -1)


def layer_kernel(n_dev, attn_scale,
                 x, dy, g1, s1, bo, g2, s2, bd, wqkv, bqkv, wo, wu, bu, wd,
                 y_out, dx_out, vec_out, dwqkv_out, dwo_out, dwu_out, dbu_out, dwd_out,
                 h1own, h1, wob, wp, wqp, wq, q_s, k_s, v_s, qkvt, big, lse, o_own, o_all, wo_all, x1, hh, dyy, ga, dza, acc, dx1,
                 do_send, do_all, do_s, delta, dqt, p_b, ds_b, dqkvt, wq_cat, dh_send, dh_pair, dh_all, dwq, dwq_r,
                 dwp, prx, frx, dwop, dwo_pr, dwo_rx, vec, vec_all,
                 hs_ss, hs_rs, hp_ss, hp_rs, wq_ss, wq_rs, wb_ss, wb_rs, o_ss, o_rs, do_ss, do_rs, dhp_ss, dhp_rs, dh_ss, dh_rs,
                 wp_ss, wp_rs, mt_ss, mt_rs, pr_ss, pr_rs, fr_ss, fr_rs, op_ss, op_rs, ox_ss, ox_rs, v_ss, v_rs):
    me = lax.axis_index("tp")
    chips = n_dev // 2
    chip, core = lax.div(me, 2), lax.rem(me, 2)
    seq = lax.div(chip, chips // 2)
    mate = 2 * (chips - 1 - chip) + core
    side = chip + 1 - 2 * lax.rem(chip, 2)
    flank, across = 2 * side + core, 2 * (chips - 1 - side) + core

    def dev(shift, other):
        return 2 * lax.rem(chip + shift + chips, chips) + (1 - core if other else core)

    PT = dev(0, True)

    def handler(n, st):
        return n if (n // 2) // (chips // 2) == st else 2 * (chips - 1 - n // 2) + n % 2

    def rc(src, dst, ssem, rsem, target):
        return pltpu.make_async_remote_copy(src_ref=src, dst_ref=dst, send_sem=ssem, recv_sem=rsem,
                                            device_id={"tp": target}, device_id_type=MESH)

    def m256(i):
        return pl.ds(i * TOK, TOK) if isinstance(i, int) else pl.ds(pl.multiple_of(i * TOK, TOK), TOK)

    def m64(i):
        return pl.ds(i * HEAD, HEAD) if isinstance(i, int) else pl.ds(pl.multiple_of(i * HEAD, HEAD), HEAD)
    barrier = pltpu.get_barrier_semaphore()
    for i in range(n_dev):
        @pl.when(me != i)
        def _():
            pl.semaphore_signal(barrier, inc=1, device_id={"tp": i}, device_id_type=MESH)

    gain1, shift1 = vector(g1), vector(s1)
    for b in range(2):
        for r in range(2):
            rows = slice(b * TOK + r * HALF, b * TOK + r * HALF + HALF)
            x_hat, _ = norm_stats(x[rows, :].astype(F32))
            h1own[b, r * HALF:r * HALF + HALF, :] = (x_hat * gain1 + shift1).astype(BF16)
    h1[m256(me), :] = h1own[seq]
    wqp[0, 0:QKV, :] = wqkv[...]
    bq_row = jnp.concatenate([bqkv[c].astype(F32) for c in range(THREE)] + [jnp.zeros((1, TAIL), F32)], axis=1)
    wqp[0, QKV:WQ_ROWS, :] = jnp.broadcast_to(bq_row, (PACK, WIDTH)).astype(BF16)

    def h1_copy(step):
        src, row, target = ((h1own.at[1 - seq], me, mate), (h1own.at[seq], me, flank), (h1.at[m256(mate), :], mate, flank))[step]
        return rc(src, h1.at[m256(row), :], hs_ss.at[step], hs_rs.at[step], target)

    def h1_recv(step, src):
        return rc(h1own.at[0], h1.at[m256(2 * src + core), :], hs_ss.at[0], hs_rs.at[step], PT)

    def h1_pair(src, received):
        rows = m256(2 * src + (1 - core if received else core))
        return rc(h1.at[rows, :], h1.at[rows, :], hp_ss.at[src], hp_rs.at[src], PT)

    def wq_copy():
        return rc(wqp.at[0], wqp.at[1], wq_ss.at[0], wq_rs.at[0], mate)
    pl.semaphore_wait(barrier, n_dev - 1)
    h1_copy(0).start()
    h1_copy(1).start()
    h1_pair(chip, False).start()
    wob[me, 0:HEAD, :] = wo[...]
    wob[me, HEAD:80, 0:TOK] = jnp.broadcast_to(vector(bu), (PACK, TOK)).astype(BF16)
    wob[me, HEAD:80, TOK:WIDTH] = jnp.zeros((PACK, TOK), BF16)
    wp[me, 0:TOK, :] = wd[...]
    wp[me, TOK:WIDTH, :] = wu[...].astype(F32).T.astype(BF16)
    dyy[0:WIDTH, :] = dy[...]

    def twin(d):
        return d + 1 - 2 * core

    w_plan = ((me, PT, PT, 0, WIDTH), (me, mate, mate, 0, TOK), (me, mate, mate, TOK, TOK), (me, flank, flank, 0, WIDTH),
              (mate, flank, across, 0, TOK), (mate, flank, across, TOK, TOK),
              (flank, PT, twin(flank), 0, WIDTH), (mate, PT, twin(mate), 0, WIDTH), (across, PT, twin(across), 0, WIDTH))

    def w_copy(step, received=False):
        own, target, got, off, size = w_plan[step]
        v = wp.at[got if received else own, pl.ds(off, size), :]
        return rc(v, v, wp_ss.at[step], wp_rs.at[step], target)

    def w_wait(*steps):
        for step in steps:
            w_copy(step, True).wait_recv()

    def w_start(*steps):
        for step in steps:
            w_copy(step).start()

    o_plan = ((me, PT, PT), (me, mate, mate), (me, flank, flank), (mate, flank, across),
              (flank, PT, twin(flank)), (mate, PT, twin(mate)), (across, PT, twin(across)))

    def wo_all_copy(step, received=False):
        own, target, got = o_plan[step]
        v = wob.at[got if received else own]
        return rc(v, v, wb_ss.at[step], wb_rs.at[step], target)

    def wo_wait(*steps):
        for step in steps:
            wo_all_copy(step, True).wait_recv()

    def wo_start(*steps):
        for step in steps:
            wo_all_copy(step).start()

    wo_start(0)

    def mate_copy(step):
        src, dst = ((hh.at[0:TOK], hh.at[WIDTH:768]), (hh.at[TOK:WIDTH], hh.at[768:1024]), (dyy.at[0:WIDTH], dyy.at[WIDTH:1024]))[step]
        return rc(src, dst, mt_ss.at[step], mt_rs.at[step], mate)

    w_start(0)

    def natural(hi):
        full = jnp.concatenate([wqp[hi, 0:QKV, :].astype(F32), jnp.zeros((HEAD, WIDTH), F32)], axis=0)
        wq[:, hi * TOK:(hi + 1) * TOK] = full.T.astype(BF16)

    natural(0)

    def project(owner, hi):
        rows = m256(owner)
        bias = wqp[hi, QKV:WQ_ROWS, 0:TOK].astype(F32)[0:1, :]
        part = (mm(h1[rows, :], wq[:, hi * TOK:(hi + 1) * TOK]) + bias).astype(BF16).astype(F32)
        q_s[hi, rows, :] = part[:, 0:HEAD].astype(BF16)
        k_s[hi, rows, :] = part[:, HEAD:HALF].astype(BF16)
        v_s[hi, rows, :] = part[:, HALF:QKV].astype(BF16)
        qkvt[hi, :, rows] = part.T[:QKV, :].astype(BF16)

    def near(t):
        base = chip + lax.div(t, 2) * (side - chip)
        return base + lax.rem(t, 2) * (chips - 1 - 2 * base)
    @pl.loop(0, chips)
    def _(t):
        src = near(t)

        @pl.when(t == 2)
        def _():
            wq_copy().start()
            wo_start(1, 2)
            w_start(1, 2, THREE)

        @pl.when(t > 0)
        def _():
            h1_recv(t - 1, src).wait_recv()
            h1_pair(src, False).start()

        @pl.when(t == 1)
        def _():
            h1_copy(2).start()

        project(2 * src + core, 0)
        h1_pair(src, True).wait_recv()
        project(2 * src + 1 - core, 0)


    s_fac = attn_scale * LOG2E
    keep = lax.broadcasted_iota(jnp.int32, (TOK, TOK), 0) <= lax.broadcasted_iota(jnp.int32, (TOK, TOK), 1)

    def o_copy(hi, j):
        head = me + hi * (mate - me)
        return rc(o_own.at[hi, :, m256(j)], o_all.at[m64(head), m256(seq)], o_ss.at[hi, j], o_rs.at[seq, head], j)

    def fold(value, op):
        return op(value.reshape(32, SUB, TOK), axis=0)

    def attend(hi, j):
        cols = m256(j)
        q_t = qkvt[hi, 0:HEAD, cols]
        base = SUB * (j % 2)
        m = jnp.full((SUB, TOK), -1e30, F32)
        for kc in range(j + 1):
            s = mm(k_s[hi, m256(kc), :], q_t) * s_fac
            if kc == j:
                s = jnp.where(keep, s, -1e30)
            big[base + kc] = s
            m = jnp.maximum(m, fold(s, jnp.max))
        m = jnp.max(m, axis=0, keepdims=True)
        l = jnp.zeros((SUB, TOK), F32)
        for kc in range(j + 1):
            l = l + fold(jnp.exp2(big[base + kc] - m), jnp.sum)
        lse_j = m + jnp.log2(jnp.sum(l, axis=0, keepdims=True))
        lse[hi, :, cols] = lse_j
        o = jnp.zeros((HEAD, TOK), F32)
        for kc in range(j + 1):
            p = jnp.exp2(big[base + kc] - lse_j).astype(BF16)
            o = o + mm(qkvt[hi, HALF:QKV, m256(kc)], p)
        o = o.astype(BF16)
        o_own[hi, :, cols] = o

        @pl.when(me != j)
        def _():
            o_copy(hi, j).start()

        @pl.when(me == j)
        def _():
            o_all[m64(me + hi * (mate - me)), m256(seq)] = o
    @pl.loop(0, 2)
    def _(hi):
        @pl.when(hi == 1)
        def _():
            wq_copy().wait_recv()
            natural(1)

            @pl.loop(0, n_dev)
            def _(owner):
                project(owner, 1)

        for j in range(n_dev):
            attend(hi, j)
            if j == 2:
                @pl.when(hi == 1)
                def _():
                    wo_wait(1)
                    wo_start(THREE, 5)
            if j == 6:
                @pl.when(hi == 1)
                def _():
                    wo_wait(2, THREE)
                    wo_start(FOUR, 6)
    mate_copy(2).start()
    w_wait(1, 2)
    w_start(FOUR, 5)
    w_wait(THREE)
    w_start(6, 7)
    wo_wait(0, FOUR, 5, 6)
    for n in range(n_dev):
        wo_all[n * HEAD:(n + 1) * HEAD, :] = wob[n, 0:HEAD, :]
    for st in range(2):
        for n in range(n_dev):
            @pl.when(me != handler(n, st))
            def _():
                rc(o_own.at[0, :, m256(0)], o_all.at[m64(n), m256(st)], o_ss.at[0, 0], o_rs.at[st, n], PT).wait_recv()

    bias_o = vector(bo)
    gain2, shift2 = vector(g2), vector(s2)
    for r in range(FOUR):
        rows = slice(r * HALF, r * HALF + HALF)
        attn = mm(o_all[:, rows], wo_all[...], 0, 0)
        x1_r = (x[rows, :].astype(F32) + attn + bias_o).astype(BF16)
        x1[rows, :] = x1_r
        x_hat, _ = norm_stats(x1_r.astype(F32))
        hh[rows, :] = (x_hat * gain2 + shift2).astype(BF16)
        if r % 2 == 1:
            mate_copy(r // 2).start()

    def mlp(n, rows):
        w2 = wp[n, 0:TOK, :]
        w1t = wp[n, TOK:WIDTH, :]
        bias_u = wob[n, HEAD:80, 0:TOK].astype(F32)[0:1, :]
        z = (mm(hh[rows, :], w1t, 1, 1) + bias_u).astype(BF16).astype(F32)
        z2 = z * z
        h = 0.5 * jnp.tanh(z * (GELU_A + GELU_AB * z2)) + 0.5
        g = z * h
        slope = h + g * ((1.0 - h) * (2.0 * GELU_A + 6.0 * GELU_AB * z2))
        dgl = mm(dyy[rows, :], w2, 1, 1).astype(BF16).astype(F32)
        dz = (dgl * slope).astype(BF16)
        ga[n, rows, :] = g.astype(BF16)
        dza[n, rows, :] = dz
        return dz, w1t

    def block(i):
        which, own = lax.div(i, 2), lax.rem(i, 2)
        return which, own, 2 * (side + which * (chip - side)) + (1 - core) + own * (2 * core - 1)

    def own_grads():
        @pl.loop(0, FOUR)
        def _(i):
            _, _, n = block(i)
            own_rows = slice(0, WIDTH)
            dwp[i, 0:TOK, :] = mm(ga[n, own_rows, :], dyy[own_rows, :], 0, 0)
            dwp[i, TOK:WIDTH, :] = mm(dza[n, own_rows, :], hh[own_rows, :], 0, 0)
            dwp[i, WIDTH:528, 0:TOK] = jnp.broadcast_to(jnp.sum(dza[n, own_rows, :].astype(F32), axis=0, keepdims=True), (PACK, TOK))
            dwp[i, WIDTH:528, TOK:WIDTH] = jnp.zeros((PACK, TOK), F32)
    acc[...] = jnp.zeros_like(acc)

    @pl.loop(0, n_dev)
    def _(i):
        t, other = lax.div(i, 2), lax.rem(i, 2)
        near_chip = chip + lax.rem(t, 2) * (side - chip)
        n = 2 * (near_chip + lax.div(t, 2) * (chips - 1 - 2 * near_chip)) + core + other * (1 - 2 * core)
        for step, at in ((0, 1), (6, THREE), (7, 5), (SUB, 7)):
            @pl.when(i == at)
            def _():
                w_wait(step)

        @pl.when(i == 6)
        def _():
            own_grads()
            w_wait(FOUR, 5)
            w_start(SUB)

        for r in range(2):
            rows = slice(r * TOK, r * TOK + TOK)
            dz, w1t = mlp(n, rows)
            acc[rows, :] += mm(dz, w1t)
    vec[...] = jnp.zeros_like(vec)
    for r in range(FOUR):
        rows = slice(r * HALF, r * HALF + HALF)
        dh2 = acc[rows, :].astype(BF16).astype(F32)
        x_hat, inv_std = norm_stats(x1[rows, :].astype(F32))
        dy_r = dy[rows, :].astype(F32)
        dx1_r = (dy_r + norm_back(dh2, x_hat, inv_std, gain2)).astype(BF16)
        dx1[rows, :] = dx1_r
        vec[2:THREE, :] += jnp.sum(dx1_r.astype(F32), axis=0, keepdims=True)
        vec[THREE:FOUR, :] += jnp.sum(dh2 * x_hat, axis=0, keepdims=True)
        vec[FOUR:5, :] += jnp.sum(dh2, axis=0, keepdims=True)
        vec[5:6, :] += jnp.sum(dy_r, axis=0, keepdims=True)

    def do_copy(n, st):
        target = handler(n, st)
        hi = 0 if target == n else 1
        return rc(do_send.at[m64(n), m256(st)], do_all.at[hi, :, m256(me)], do_ss.at[n, st], do_rs.at[hi, me], target)

    for r in range(2):
        rows = slice(r * TOK, r * TOK + TOK)
        do_send[rows, :] = mm(wo_all[rows, :], dx1[...], 1, 1).astype(BF16)
    def wo_pair_copy(slot):
        return rc(dwop.at[2 * slot + 1 - core], dwo_pr.at[slot], op_ss.at[slot], op_rs.at[slot], PT)

    def wo_copy(t):
        return rc(dwop.at[2 * t + core], dwo_rx.at[chip], ox_ss.at[t], ox_rs.at[chip], 2 * t + core)
    for n in range(n_dev):
        dwop[n] = mm(o_all[m64(n), :], dx1[...])
    for t in range(chips):
        wo_pair_copy(t).start()

    def pair_copy(which):
        return rc(dwp.at[2 * which], prx.at[which], pr_ss.at[which], pr_rs.at[which], PT)

    def side_copy(step):
        rows = pl.ds(step * (G_ROWS // THREE), G_ROWS // THREE)
        return rc(dwp.at[1, rows], frx.at[rows], fr_ss.at[step], fr_rs.at[step], flank)

    def pair_add(which):
        pair_copy(which).wait_recv()
        dwp[2 * which + 1] += prx[which]

    for t in range(chips):
        wo_pair_copy(t).wait_recv()
        dwop[2 * t + core] += dwo_pr[t]

    wo_copy(side).start()
    mate_copy(2).wait_recv()
    for r in range(2):
        mate_copy(r).wait_recv()
        rows = slice(WIDTH + r * TOK, 768 + r * TOK)
        if r == 1:
            for n in range(n_dev):
                for st in range(2):
                    @pl.when(me != handler(n, st))
                    def _():
                        do_copy(n, st).start()

                    @pl.when(me == handler(n, st))
                    def _():
                        do_all[0 if handler(n, st) == n else 1, :, m256(me)] = do_send[m64(n), m256(st)]
        @pl.loop(0, FOUR)
        def _(i):
            which, own, n = block(i)
            mlp(n, rows)
            dwp[i, 0:TOK, :] += mm(ga[n, rows, :], dyy[rows, :], 0, 0)
            dwp[i, TOK:WIDTH, :] += mm(dza[n, rows, :], hh[rows, :], 0, 0)
            dwp[i, WIDTH:528, 0:TOK] += jnp.broadcast_to(jnp.sum(dza[n, rows, :].astype(F32), axis=0, keepdims=True), (PACK, TOK))
            if r == 1:
                @pl.when(own == 0)
                def _():
                    pair_copy(which).start()

                @pl.when(i == 2)
                def _():
                    pair_add(0)
                    for step in range(2):
                        side_copy(step).start()

    pair_add(1)

    for j in range(n_dev):
        for hi in range(2):
            @pl.when(me != j)
            def _():
                rc(do_send.at[m64(0), m256(0)], do_all.at[hi, :, m256(j)], do_ss.at[0, 0], do_rs.at[hi, j], PT).wait_recv()
            do_t = do_all[hi, :, m256(j)].astype(F32)
            do_s[hi, m256(j), :] = do_t.T.astype(BF16)
            delta[hi, :, m256(j)] = jnp.sum(do_t * o_own[hi, :, m256(j)].astype(F32), axis=0, keepdims=True)
    for t in range(chips):
        @pl.when((chip != t) & (side != t))
        def _():
            wo_copy(t).start()
    dwq[...] = jnp.zeros_like(dwq)
    for hi in range(2):
        wq_cat[hi * QKV:(hi + 1) * QKV, :] = wqp[hi, 0:QKV, :]

    def dwq_copy():
        return rc(dwq.at[1], dwq_r, wq_ss.at[1], wq_rs.at[1], mate)

    def dh_pair_copy(kb):
        return rc(dh_send.at[kb], dh_pair.at[kb // 2], dhp_ss.at[kb // 2], dhp_rs.at[kb // 2], PT)

    def dh_copy(kb):
        return rc(dh_send.at[kb], dh_all.at[chip], dh_ss.at[kb // 2], dh_rs.at[chip], kb)

    def dh_finish(kb):
        @pl.when(core == kb % 2)
        def _():
            dh_pair_copy(kb).wait_recv()
            total = (dh_send[kb].astype(F32) + dh_pair[kb // 2].astype(F32)).astype(BF16)
            dh_send[kb] = total

            @pl.when(me != kb)
            def _():
                dh_copy(kb).start()

            @pl.when(me == kb)
            def _():
                dh_all[chip] = total
    @pl.loop(0, 2)
    def _(i):
        hi = 1 - i
        base = pl.multiple_of(QKV * hi, HEAD)

        @pl.when(i == 1)
        def _():
            dwq_copy().start()

        for kb in range(n_dev):
            rows = m256(kb)
            late = slice(kb * TOK, n_dev * TOK)
            for qb in range(kb, n_dev):
                cols = m256(qb)
                for c in range(2):
                    part = slice(c * HALF, c * HALF + HALF)
                    keys = slice(kb * TOK + c * HALF, kb * TOK + c * HALF + HALF)
                    p = jnp.exp2(mm(k_s[hi, keys, :], qkvt[hi, 0:HEAD, cols]) * s_fac - lse[hi, :, cols])
                    if qb == kb:
                        p = jnp.where(keep[part], p, 0.0)
                    dp = mm(v_s[hi, keys, :], do_all[hi, :, cols]).astype(BF16).astype(F32)
                    p_b[kb % 2, part, cols] = p.astype(BF16)
                    ds_b[kb % 2, part, cols] = (p * (dp - delta[hi, :, cols])).astype(BF16)
            dv = mm(p_b[kb % 2, :, late], do_s[hi, late, :])
            dk = mm(ds_b[kb % 2, :, late], q_s[hi, late, :]) * attn_scale
            dq = mm(qkvt[hi, HEAD:HALF, rows], ds_b[kb % 2, :, late])
            if kb == 0:
                dqt[...] = dq
            else:
                dqt[:, late] += dq
            dqkvt[pl.ds(base, HEAD), rows] = (dqt[:, rows] * attn_scale).astype(BF16)
            dqkvt[pl.ds(base + HEAD, HALF), rows] = jnp.concatenate([dk, dv], axis=1).T.astype(BF16)

            @pl.when(i == 1)
            def _():
                dh = mm(dqkvt[:, rows], wq_cat[...], 0, 0)
                dh_send[kb] = dh.astype(BF16)

                @pl.when(core != kb % 2)
                def _():
                    dh_pair_copy(kb).start()

                if kb > 0:
                    dh_finish(kb - 1)


        mine = dqkvt[pl.ds(base, QKV), :]
        dwq[hi, 0:QKV, :] = mm(mine, h1[...])
        dwq[hi, QKV:DW_ROWS, 0:QKV] = mm(jnp.ones((SUB, SEQ), BF16), mine, 1, 1)

    dh_finish(n_dev - 1)
    side_copy(2).start()

    acc[...] = jnp.zeros_like(acc)

    @pl.loop(0, n_dev)
    def _(n):
        for r in range(2):
            rows = slice(r * TOK, r * TOK + TOK)
            acc[rows, :] += mm(ga[n, rows, :], wp[n, 0:TOK, :])

    y_out[...] = (x1[...].astype(F32) + acc[...] + vector(bd)).astype(BF16)

    for t in range(chips):
        @pl.when(chip != t)
        def _():
            rc(dh_send.at[0], dh_all.at[t], dh_ss.at[0], dh_rs.at[t], PT).wait_recv()
    for r in range(FOUR):
        rows = slice(r * HALF, r * HALF + HALF)
        half = slice((r % 2) * HALF, (r % 2) * HALF + HALF)
        first = (r // 2) * (chips // 2)
        dh1 = (dh_all[first, half, :].astype(F32) + dh_all[first + 1, half, :].astype(F32)).astype(BF16).astype(F32)
        x_hat, inv_std = norm_stats(x[rows, :].astype(F32))
        dx_out[rows, :] = (dx1[rows, :].astype(F32) + norm_back(dh1, x_hat, inv_std, gain1)).astype(BF16)
        vec[0:1, :] += jnp.sum(dh1 * x_hat, axis=0, keepdims=True)
        vec[1:2, :] += jnp.sum(dh1, axis=0, keepdims=True)

    def vec_copy(j):
        return rc(vec, vec_all.at[me], v_ss.at[j], v_rs.at[me], j)
    for j in range(n_dev):
        @pl.when(me != j)
        def _():
            vec_copy(j).start()
    vec_all[me] = vec[...]
    for step in range(THREE):
        side_copy(step).wait_recv()
    dwd_out[...] = dwp[THREE, 0:TOK, :] + frx[0:TOK, :]
    dwu_out[...] = (dwp[THREE, TOK:WIDTH, :] + frx[TOK:WIDTH, :]).T
    dbu_out[...] = dwp[THREE, WIDTH:520, 0:TOK] + frx[WIDTH:520, 0:TOK]
    dwo_rx[chip] = dwop[me]
    for t in range(chips):
        @pl.when(chip != t)
        def _():
            rc(dwop.at[0], dwo_rx.at[t], ox_ss.at[0], ox_rs.at[t], PT).wait_recv()
    dwo_out[...] = dwo_rx[0] + dwo_rx[1] + dwo_rx[2] + dwo_rx[THREE]

    dwq_copy().wait_recv()
    dwqkv_out[...] = dwq[0] + dwq_r[...]
    for j in range(n_dev):
        @pl.when(me != j)
        def _():
            rc(vec, vec_all.at[j], v_ss.at[0], v_rs.at[j], PT).wait_recv()
    total = vec_all[0]
    for j in range(1, n_dev):
        total = total + vec_all[j]
    vec_out[...] = total

    wq_copy().wait_send()
    dwq_copy().wait_send()
    for t in range(chips):
        h1_pair(t, False).wait_send()

        @pl.when(chip != t)
        def _():
            wo_copy(t).wait_send()

        wo_pair_copy(t).wait_send()
    for step in range(9):
        w_copy(step).wait_send()
    for step in range(7):
        wo_all_copy(step).wait_send()
    for step in range(THREE):
        h1_copy(step).wait_send()
    for step in range(THREE):
        mate_copy(step).wait_send()
    for which in range(2):
        pair_copy(which).wait_send()
    for step in range(THREE):
        side_copy(step).wait_send()
    for j in range(n_dev):
        @pl.when(me != j)
        def _():
            vec_copy(j).wait_send()
            for hi in range(2):
                o_copy(hi, j).wait_send()

        for st in range(2):
            @pl.when(me != handler(j, st))
            def _():
                do_copy(j, st).wait_send()

        @pl.when(core != j % 2)
        def _():
            dh_pair_copy(j).wait_send()

        @pl.when((core == j % 2) & (me != j))
        def _():
            dh_copy(j).wait_send()


def finish_kernel(y, dx, vec, dwqkv, dwo, dwu, dbu, dwd, y_o, dx_o, v0, v1, dwqkv_o, dbqkv_o, dwo_o, v2, v3, v4, dwu_o, dbu_o, dwd_o, v5):
    y_o[...] = y[...]
    dx_o[...] = dx[...]
    for i, ref in enumerate((v0, v1, v2, v3, v4, v5)):
        ref[...] = vec[i:i + 1, :].reshape(ref.shape)
    dwqkv_o[...] = dwqkv[0:QKV, :]
    for c in range(THREE):
        dbqkv_o[c] = dwqkv[QKV:193, c * HEAD:(c + 1) * HEAD]
    dwo_o[...] = dwo[...]
    dwu_o[...] = dwu[...]
    dbu_o[...] = dbu[0:1, :].reshape(dbu_o.shape)
    dwd_o[...] = dwd[...]


def solution(mesh):
    n_dev = mesh.shape["tp"]

    def device_step(hidden, grad_out, ln1_gain, ln1_bias, w_qkv, b_qkv, w_out, b_out, ln2_gain, ln2_bias, w_up, b_up, w_down, b_down):
        batch, tokens, d = hidden.shape
        rows = batch * tokens
        head = w_qkv.shape[-1]
        seq = tokens * n_dev
        ff = w_up.shape[1]
        chips = n_dev // 2
        attn_scale = head ** -0.5
        sds = jax.ShapeDtypeStruct
        vm = pltpu.VMEM

        def dma(*shape):
            return pltpu.SemaphoreType.DMA(shape)

        vspec = pl.BlockSpec(memory_space=pltpu.VMEM)
        outs = pl.pallas_call(
            lambda *refs: layer_kernel(n_dev, attn_scale, *refs),
            out_shape=(sds((rows, d), BF16), sds((rows, d), BF16), sds((SUB, d), F32), sds((DW_ROWS, d), F32),
                       sds((head, d), F32), sds((d, ff), F32), sds((SUB, ff), F32), sds((ff, d), F32)),
            in_specs=[vspec] * 14,
            out_specs=tuple([vspec] * SUB),
            scratch_shapes=[
                vm((2, tokens, d), BF16), vm((seq, d), BF16), vm((n_dev, WO_ROWS, d), BF16), vm((n_dev, 2 * ff, d), BF16),
                vm((2, WQ_ROWS, d), BF16), vm((d, WIDTH), BF16),
                vm((2, seq, head), BF16), vm((2, seq, head), BF16), vm((2, seq, head), BF16), vm((2, THREE * head, seq), BF16),
                vm((PACK, TOK, TOK), F32), vm((2, 1, seq), F32), vm((2, head, seq), BF16), vm((n_dev * head, rows), BF16),
                vm((n_dev * head, d), BF16), vm((rows, d), BF16), vm((2 * rows, d), BF16), vm((2 * rows, d), BF16),
                vm((n_dev, 2 * rows, ff), BF16), vm((n_dev, 2 * rows, ff), BF16), vm((rows, d), F32), vm((rows, d), BF16),
                vm((n_dev * head, rows), BF16), vm((2, head, seq), BF16), vm((2, seq, head), BF16),
                vm((2, 1, seq), F32), vm((head, seq), F32), vm((2, TOK, seq), BF16), vm((2, TOK, seq), BF16), vm((6 * head, seq), BF16), vm((6 * head, d), BF16),
                vm((n_dev, tokens, d), BF16), vm((chips, tokens, d), BF16), vm((chips, tokens, d), BF16),
                vm((2, DW_ROWS, d), F32), vm((DW_ROWS, d), F32),
                vm((FOUR, G_ROWS, d), F32), vm((2, G_ROWS, d), F32), vm((G_ROWS, d), F32),
                vm((n_dev, head, d), F32), vm((chips, head, d), F32), vm((chips, head, d), F32),
                vm((SUB, d), F32), vm((n_dev, SUB, d), F32),
                dma(chips), dma(chips), dma(chips), dma(chips), dma(2), dma(2), dma(7), dma(7), dma(2, n_dev), dma(2, n_dev),
                dma(n_dev, 2), dma(2, n_dev), dma(chips), dma(chips), dma(chips), dma(chips),
                dma(9), dma(9), dma(THREE), dma(THREE), dma(2), dma(2), dma(THREE), dma(THREE), dma(chips), dma(chips), dma(chips), dma(chips), dma(n_dev), dma(n_dev),
            ],
            compiler_params=pltpu.CompilerParams(collective_id=0, has_side_effects=True, vmem_limit_bytes=67043328),
            name="layer",
        )(hidden.reshape(rows, d), grad_out.reshape(rows, d), ln1_gain, ln1_bias, b_out, ln2_gain, ln2_bias, b_down,
          w_qkv.transpose(1, 2, THREE, 0).reshape(THREE * head, d), b_qkv, w_out.reshape(head, d), w_up, b_up, w_down)
        v1d = sds((d,), F32)
        y, dx, v0, v1, dwqkv_t, dbqkv, dwo, v2, v3, v4, dwu, dbu, dwd, v5 = pl.pallas_call(
            finish_kernel,
            out_shape=(sds((rows, d), BF16), sds((rows, d), BF16), v1d, v1d, sds((THREE * head, d), F32), sds((THREE, 1, head), F32),
                       sds((head, d), F32), v1d, v1d, v1d, sds((d, ff), F32), sds((ff,), F32), sds((ff, d), F32), v1d),
            in_specs=[vspec] * SUB,
            out_specs=tuple([vspec] * 14),
            name="finish",
        )(*outs)
        return (y.reshape(hidden.shape), dx.reshape(hidden.shape), v0, v1, dwqkv_t.reshape(THREE, 1, head, d).transpose(THREE, 0, 1, 2),
                dbqkv, dwo.reshape(w_out.shape), v2, v3, v4, dwu, dbu, dwd, v5)

    act_spec = P("dp", "tp", None)
    vec_spec = P(None)
    group_vec = P("dp")
    in_specs = (act_spec, act_spec, vec_spec, vec_spec, P(None, None, "tp", None), P(None, "tp", None), P("tp", None, None), vec_spec, vec_spec, vec_spec, P(None, "tp"), P("tp"), P("tp", None), vec_spec)
    out_specs = (act_spec, act_spec, group_vec, group_vec, P("dp", None, "tp", None), P("dp", "tp", None), P(("dp", "tp"), None, None), group_vec, group_vec, group_vec, P("dp", "tp"), P(("dp", "tp")), P(("dp", "tp"), None), group_vec)
    return jax.shard_map(device_step, mesh=mesh, in_specs=in_specs, out_specs=out_specs, check_vma=False)
```

```python
import jax
import jax.numpy as jnp
from jax import lax
from jax.experimental import pallas as pl
from jax.experimental.pallas import tpu as pltpu
from jax.sharding import PartitionSpec as P

LN_EPS = 1e-5
MESH = pl.DeviceIdType.MESH
F32 = jnp.float32
BF16 = jnp.bfloat16
LOG2E = 1.4426950408889634
GELU_A = 0.7978845608028654
GELU_AB = GELU_A * 0.044715

TOK = 256
WIDTH = 512
HEAD = 64
HALF = 128
QKV = 192
SUB = 8
TAIL = 320
WQ_ROWS = 208
PACK = 16
THREE = 3
DW_ROWS = 200
SEQ = 2048
FOUR = 4
WO_ROWS = 80
G_ROWS = 528


def mm(lhs, rhs, lc=1, rc=0):
    return lax.dot_general(lhs, rhs, (((lc,), (rc,)), ((), ())), preferred_element_type=F32)


def norm_stats(value):
    centered = value - jnp.mean(value, axis=-1, keepdims=True)
    inv_std = lax.rsqrt(jnp.mean(centered * centered, axis=-1, keepdims=True) + LN_EPS)
    return centered * inv_std, inv_std


def norm_back(grad, x_hat, inv_std, gain):
    scaled = grad * gain
    return inv_std * (scaled - jnp.mean(scaled, axis=-1, keepdims=True) - x_hat * jnp.mean(scaled * x_hat, axis=-1, keepdims=True))


def vector(ref):
    return ref[...].astype(F32).reshape(1, -1)


def layer_kernel(n_dev, attn_scale,
                 x, dy, g1, s1, bo, g2, s2, bd, wqkv, bqkv, wo, wu, bu, wd,
                 y_out, dx_out, vec_out, dwqkv_out, dwo_out, dwu_out, dbu_out, dwd_out,
                 h1own, h1, wob, wp, wqp, wq, q_s, k_s, v_s, qkvt, big, lse, o_own, o_all, wo_all, x1, hh, dyy, ga, dza, acc, dx1,
                 do_send, do_all, do_s, delta, dqt, p_b, ds_b, p_f, dqkvt, wq_cat, dh_send, dh_pair, dh_all, dwq, dwq_r,
                 dwp, prx, frx, dwop, dwo_pr, dwo_rx, vec, vec_all,
                 hs_ss, hs_rs, hp_ss, hp_rs, wq_ss, wq_rs, wb_ss, wb_rs, o_ss, o_rs, do_ss, do_rs, dhp_ss, dhp_rs, dh_ss, dh_rs,
                 wp_ss, wp_rs, mt_ss, mt_rs, pr_ss, pr_rs, fr_ss, fr_rs, op_ss, op_rs, ox_ss, ox_rs, v_ss, v_rs):
    me = lax.axis_index("tp")
    chips = n_dev // 2
    chip, core = lax.div(me, 2), lax.rem(me, 2)
    seq = lax.div(chip, chips // 2)
    mate = 2 * (chips - 1 - chip) + core
    side = chip + 1 - 2 * lax.rem(chip, 2)
    flank, across = 2 * side + core, 2 * (chips - 1 - side) + core

    def dev(shift, other):
        return 2 * lax.rem(chip + shift + chips, chips) + (1 - core if other else core)

    PT = dev(0, True)

    def handler(n, st):
        return n if (n // 2) // (chips // 2) == st else 2 * (chips - 1 - n // 2) + n % 2

    def rc(src, dst, ssem, rsem, target):
        return pltpu.make_async_remote_copy(src_ref=src, dst_ref=dst, send_sem=ssem, recv_sem=rsem,
                                            device_id={"tp": target}, device_id_type=MESH)

    def m256(i):
        return pl.ds(i * TOK, TOK) if isinstance(i, int) else pl.ds(pl.multiple_of(i * TOK, TOK), TOK)

    def m64(i):
        return pl.ds(i * HEAD, HEAD) if isinstance(i, int) else pl.ds(pl.multiple_of(i * HEAD, HEAD), HEAD)
    barrier = pltpu.get_barrier_semaphore()
    for i in range(n_dev):
        @pl.when(me != i)
        def _():
            pl.semaphore_signal(barrier, inc=1, device_id={"tp": i}, device_id_type=MESH)

    gain1, shift1 = vector(g1), vector(s1)
    for b in range(2):
        for r in range(2):
            rows = slice(b * TOK + r * HALF, b * TOK + r * HALF + HALF)
            x_hat, _ = norm_stats(x[rows, :].astype(F32))
            h1own[b, r * HALF:r * HALF + HALF, :] = (x_hat * gain1 + shift1).astype(BF16)
    h1[m256(me), :] = h1own[seq]
    wqp[0, 0:QKV, :] = wqkv[...]
    bq_row = jnp.concatenate([bqkv[c].astype(F32) for c in range(THREE)] + [jnp.zeros((1, TAIL), F32)], axis=1)
    wqp[0, QKV:WQ_ROWS, :] = jnp.broadcast_to(bq_row, (PACK, WIDTH)).astype(BF16)

    def h1_copy(step):
        src, row, target = ((h1own.at[1 - seq], me, mate), (h1own.at[seq], me, flank), (h1.at[m256(mate), :], mate, flank))[step]
        return rc(src, h1.at[m256(row), :], hs_ss.at[step], hs_rs.at[step], target)

    def h1_recv(step, src):
        return rc(h1own.at[0], h1.at[m256(2 * src + core), :], hs_ss.at[0], hs_rs.at[step], PT)

    def h1_pair(src, received):
        rows = m256(2 * src + (1 - core if received else core))
        return rc(h1.at[rows, :], h1.at[rows, :], hp_ss.at[src], hp_rs.at[src], PT)

    def wq_copy():
        return rc(wqp.at[0], wqp.at[1], wq_ss.at[0], wq_rs.at[0], mate)
    pl.semaphore_wait(barrier, n_dev - 1)
    h1_copy(0).start()
    h1_copy(1).start()
    h1_pair(chip, False).start()
    wob[me, 0:HEAD, :] = wo[...]
    wob[me, HEAD:80, 0:TOK] = jnp.broadcast_to(vector(bu), (PACK, TOK)).astype(BF16)
    wob[me, HEAD:80, TOK:WIDTH] = jnp.zeros((PACK, TOK), BF16)
    wp[me, 0:TOK, :] = wd[...]
    wp[me, TOK:WIDTH, :] = wu[...].astype(F32).T.astype(BF16)
    dyy[0:WIDTH, :] = dy[...]

    def twin(d):
        return d + 1 - 2 * core

    w_plan = ((me, PT, PT, 0, WIDTH), (me, mate, mate, 0, TOK), (me, mate, mate, TOK, TOK), (me, flank, flank, 0, WIDTH),
              (mate, flank, across, 0, TOK), (mate, flank, across, TOK, TOK),
              (flank, PT, twin(flank), 0, WIDTH), (mate, PT, twin(mate), 0, WIDTH), (across, PT, twin(across), 0, WIDTH))

    def w_copy(step, received=False):
        own, target, got, off, size = w_plan[step]
        v = wp.at[got if received else own, pl.ds(off, size), :]
        return rc(v, v, wp_ss.at[step], wp_rs.at[step], target)

    def w_wait(*steps):
        for step in steps:
            w_copy(step, True).wait_recv()

    def w_start(*steps):
        for step in steps:
            w_copy(step).start()

    o_plan = ((me, PT, PT), (me, mate, mate), (me, flank, flank), (mate, flank, across),
              (flank, PT, twin(flank)), (mate, PT, twin(mate)), (across, PT, twin(across)))

    def wo_all_copy(step, received=False):
        own, target, got = o_plan[step]
        v = wob.at[got if received else own]
        return rc(v, v, wb_ss.at[step], wb_rs.at[step], target)

    def wo_wait(*steps):
        for step in steps:
            wo_all_copy(step, True).wait_recv()

    def wo_start(*steps):
        for step in steps:
            wo_all_copy(step).start()

    wo_start(0)

    def mate_copy(step):
        src, dst = ((hh.at[0:TOK], hh.at[WIDTH:768]), (hh.at[TOK:WIDTH], hh.at[768:1024]), (dyy.at[0:WIDTH], dyy.at[WIDTH:1024]))[step]
        return rc(src, dst, mt_ss.at[step], mt_rs.at[step], mate)

    w_start(0)

    def natural(hi):
        full = jnp.concatenate([wqp[hi, 0:QKV, :].astype(F32), jnp.zeros((HEAD, WIDTH), F32)], axis=0)
        wq[:, hi * TOK:(hi + 1) * TOK] = full.T.astype(BF16)

    natural(0)

    def project(owner, hi):
        rows = m256(owner)
        bias = wqp[hi, QKV:WQ_ROWS, 0:TOK].astype(F32)[0:1, :]
        part = (mm(h1[rows, :], wq[:, hi * TOK:(hi + 1) * TOK]) + bias).astype(BF16).astype(F32)
        q_s[hi, rows, :] = part[:, 0:HEAD].astype(BF16)
        k_s[hi, rows, :] = part[:, HEAD:HALF].astype(BF16)
        v_s[hi, rows, :] = part[:, HALF:QKV].astype(BF16)
        qkvt[hi, :, rows] = part.T[:QKV, :].astype(BF16)

    def near(t):
        base = chip + lax.div(t, 2) * (side - chip)
        return base + lax.rem(t, 2) * (chips - 1 - 2 * base)
    @pl.loop(0, chips)
    def _(t):
        src = near(t)

        @pl.when(t == 2)
        def _():
            wq_copy().start()
            wo_start(1, 2)
            w_start(1, 2, THREE)

        @pl.when(t > 0)
        def _():
            h1_recv(t - 1, src).wait_recv()
            h1_pair(src, False).start()

        @pl.when(t == 1)
        def _():
            h1_copy(2).start()

        project(2 * src + core, 0)
        h1_pair(src, True).wait_recv()
        project(2 * src + 1 - core, 0)


    s_fac = attn_scale * LOG2E
    keep = lax.broadcasted_iota(jnp.int32, (TOK, TOK), 0) <= lax.broadcasted_iota(jnp.int32, (TOK, TOK), 1)

    def o_copy(hi, j):
        head = me + hi * (mate - me)
        return rc(o_own.at[hi, :, m256(j)], o_all.at[m64(head), m256(seq)], o_ss.at[hi, j], o_rs.at[seq, head], j)

    def fold(value, op):
        return op(value.reshape(32, SUB, TOK), axis=0)

    def attend(hi, j):
        cols = m256(j)
        q_t = qkvt[hi, 0:HEAD, cols]
        base = SUB * (j % 2)
        m = jnp.full((SUB, TOK), -1e30, F32)
        for kc in range(j + 1):
            s = mm(k_s[hi, m256(kc), :], q_t) * s_fac
            if kc == j:
                s = jnp.where(keep, s, -1e30)
            big[base + kc] = s
            m = jnp.maximum(m, fold(s, jnp.max))
        m = jnp.max(m, axis=0, keepdims=True)
        l = jnp.zeros((SUB, TOK), F32)
        for kc in range(j + 1):
            l = l + fold(jnp.exp2(big[base + kc] - m), jnp.sum)
        lse_j = m + jnp.log2(jnp.sum(l, axis=0, keepdims=True))
        lse[hi, :, cols] = lse_j
        for kc in range(j + 1):
            p_f[j % 2, m256(kc), :] = jnp.exp2(big[base + kc] - lse_j).astype(BF16)
        seen = slice(0, (j + 1) * TOK)
        o = mm(qkvt[hi, HALF:QKV, seen], p_f[j % 2, seen, :])
        o = o.astype(BF16)
        o_own[hi, :, cols] = o

        @pl.when(me != j)
        def _():
            o_copy(hi, j).start()

        @pl.when(me == j)
        def _():
            o_all[m64(me + hi * (mate - me)), m256(seq)] = o
    @pl.loop(0, 2)
    def _(hi):
        @pl.when(hi == 1)
        def _():
            wq_copy().wait_recv()
            natural(1)

            @pl.loop(0, n_dev)
            def _(owner):
                project(owner, 1)

        for j in range(n_dev):
            attend(hi, j)
            if j == 2:
                @pl.when(hi == 1)
                def _():
                    wo_wait(1)
                    wo_start(THREE, 5)
            if j == 6:
                @pl.when(hi == 1)
                def _():
                    wo_wait(2, THREE)
                    wo_start(FOUR, 6)
    mate_copy(2).start()
    w_wait(1, 2)
    w_start(FOUR, 5)
    w_wait(THREE)
    w_start(6, 7)
    wo_wait(0, FOUR, 5, 6)
    for n in range(n_dev):
        wo_all[n * HEAD:(n + 1) * HEAD, :] = wob[n, 0:HEAD, :]
    for st in range(2):
        for n in range(n_dev):
            @pl.when(me != handler(n, st))
            def _():
                rc(o_own.at[0, :, m256(0)], o_all.at[m64(n), m256(st)], o_ss.at[0, 0], o_rs.at[st, n], PT).wait_recv()

    bias_o = vector(bo)
    gain2, shift2 = vector(g2), vector(s2)
    for r in range(FOUR):
        rows = slice(r * HALF, r * HALF + HALF)
        attn = mm(o_all[:, rows], wo_all[...], 0, 0)
        x1_r = (x[rows, :].astype(F32) + attn + bias_o).astype(BF16)
        x1[rows, :] = x1_r
        x_hat, _ = norm_stats(x1_r.astype(F32))
        hh[rows, :] = (x_hat * gain2 + shift2).astype(BF16)
        if r % 2 == 1:
            mate_copy(r // 2).start()

    def mlp(n, rows):
        w2 = wp[n, 0:TOK, :]
        w1t = wp[n, TOK:WIDTH, :]
        bias_u = wob[n, HEAD:80, 0:TOK].astype(F32)[0:1, :]
        z = (mm(hh[rows, :], w1t, 1, 1) + bias_u).astype(BF16).astype(F32)
        z2 = z * z
        h = 0.5 * jnp.tanh(z * (GELU_A + GELU_AB * z2)) + 0.5
        g = z * h
        slope = h + g * ((1.0 - h) * (2.0 * GELU_A + 6.0 * GELU_AB * z2))
        dgl = mm(dyy[rows, :], w2, 1, 1).astype(BF16).astype(F32)
        dz = (dgl * slope).astype(BF16)
        ga[n, rows, :] = g.astype(BF16)
        dza[n, rows, :] = dz
        return dz, w1t

    def block(i):
        which, own = lax.div(i, 2), lax.rem(i, 2)
        return which, own, 2 * (side + which * (chip - side)) + (1 - core) + own * (2 * core - 1)

    def own_grads():
        @pl.loop(0, FOUR)
        def _(i):
            _, _, n = block(i)
            own_rows = slice(0, WIDTH)
            dwp[i, 0:TOK, :] = mm(ga[n, own_rows, :], dyy[own_rows, :], 0, 0)
            dwp[i, TOK:WIDTH, :] = mm(dza[n, own_rows, :], hh[own_rows, :], 0, 0)
            dwp[i, WIDTH:528, 0:TOK] = jnp.broadcast_to(jnp.sum(dza[n, own_rows, :].astype(F32), axis=0, keepdims=True), (PACK, TOK))
            dwp[i, WIDTH:528, TOK:WIDTH] = jnp.zeros((PACK, TOK), F32)
    acc[...] = jnp.zeros_like(acc)

    @pl.loop(0, n_dev)
    def _(i):
        t, other = lax.div(i, 2), lax.rem(i, 2)
        near_chip = chip + lax.rem(t, 2) * (side - chip)
        n = 2 * (near_chip + lax.div(t, 2) * (chips - 1 - 2 * near_chip)) + core + other * (1 - 2 * core)
        for step, at in ((0, 1), (6, THREE), (7, 5), (SUB, 7)):
            @pl.when(i == at)
            def _():
                w_wait(step)

        @pl.when(i == 6)
        def _():
            own_grads()
            w_wait(FOUR, 5)
            w_start(SUB)

        for r in range(2):
            rows = slice(r * TOK, r * TOK + TOK)
            dz, w1t = mlp(n, rows)
            acc[rows, :] += mm(dz, w1t)
    vec[...] = jnp.zeros_like(vec)
    for r in range(FOUR):
        rows = slice(r * HALF, r * HALF + HALF)
        dh2 = acc[rows, :].astype(BF16).astype(F32)
        x_hat, inv_std = norm_stats(x1[rows, :].astype(F32))
        dy_r = dy[rows, :].astype(F32)
        dx1_r = (dy_r + norm_back(dh2, x_hat, inv_std, gain2)).astype(BF16)
        dx1[rows, :] = dx1_r
        vec[2:THREE, :] += jnp.sum(dx1_r.astype(F32), axis=0, keepdims=True)
        vec[THREE:FOUR, :] += jnp.sum(dh2 * x_hat, axis=0, keepdims=True)
        vec[FOUR:5, :] += jnp.sum(dh2, axis=0, keepdims=True)
        vec[5:6, :] += jnp.sum(dy_r, axis=0, keepdims=True)

    def do_copy(n, st):
        target = handler(n, st)
        hi = 0 if target == n else 1
        return rc(do_send.at[m64(n), m256(st)], do_all.at[hi, :, m256(me)], do_ss.at[n, st], do_rs.at[hi, me], target)

    for r in range(2):
        rows = slice(r * TOK, r * TOK + TOK)
        do_send[rows, :] = mm(wo_all[rows, :], dx1[...], 1, 1).astype(BF16)
    def wo_pair_copy(slot):
        return rc(dwop.at[2 * slot + 1 - core], dwo_pr.at[slot], op_ss.at[slot], op_rs.at[slot], PT)

    def wo_copy(t):
        return rc(dwop.at[2 * t + core], dwo_rx.at[chip], ox_ss.at[t], ox_rs.at[chip], 2 * t + core)
    for n in range(n_dev):
        dwop[n] = mm(o_all[m64(n), :], dx1[...])
    for t in range(chips):
        wo_pair_copy(t).start()

    def pair_copy(which):
        return rc(dwp.at[2 * which], prx.at[which], pr_ss.at[which], pr_rs.at[which], PT)

    def side_copy(step):
        rows = pl.ds(step * (G_ROWS // THREE), G_ROWS // THREE)
        return rc(dwp.at[1, rows], frx.at[rows], fr_ss.at[step], fr_rs.at[step], flank)

    def pair_add(which):
        pair_copy(which).wait_recv()
        dwp[2 * which + 1] += prx[which]

    for t in range(chips):
        wo_pair_copy(t).wait_recv()
        dwop[2 * t + core] += dwo_pr[t]

    wo_copy(side).start()
    mate_copy(2).wait_recv()
    for r in range(2):
        mate_copy(r).wait_recv()
        rows = slice(WIDTH + r * TOK, 768 + r * TOK)
        if r == 1:
            for n in range(n_dev):
                for st in range(2):
                    @pl.when(me != handler(n, st))
                    def _():
                        do_copy(n, st).start()

                    @pl.when(me == handler(n, st))
                    def _():
                        do_all[0 if handler(n, st) == n else 1, :, m256(me)] = do_send[m64(n), m256(st)]
        @pl.loop(0, FOUR)
        def _(i):
            which, own, n = block(i)
            mlp(n, rows)
            dwp[i, 0:TOK, :] += mm(ga[n, rows, :], dyy[rows, :], 0, 0)
            dwp[i, TOK:WIDTH, :] += mm(dza[n, rows, :], hh[rows, :], 0, 0)
            dwp[i, WIDTH:528, 0:TOK] += jnp.broadcast_to(jnp.sum(dza[n, rows, :].astype(F32), axis=0, keepdims=True), (PACK, TOK))
            if r == 1:
                @pl.when(own == 0)
                def _():
                    pair_copy(which).start()

                @pl.when(i == 2)
                def _():
                    pair_add(0)
                    for step in range(2):
                        side_copy(step).start()

    pair_add(1)

    for j in range(n_dev):
        for hi in range(2):
            @pl.when(me != j)
            def _():
                rc(do_send.at[m64(0), m256(0)], do_all.at[hi, :, m256(j)], do_ss.at[0, 0], do_rs.at[hi, j], PT).wait_recv()
            do_t = do_all[hi, :, m256(j)].astype(F32)
            do_s[hi, m256(j), :] = do_t.T.astype(BF16)
            delta[hi, :, m256(j)] = jnp.sum(do_t * o_own[hi, :, m256(j)].astype(F32), axis=0, keepdims=True)
    for t in range(chips):
        @pl.when((chip != t) & (side != t))
        def _():
            wo_copy(t).start()
    dwq[...] = jnp.zeros_like(dwq)
    for hi in range(2):
        wq_cat[hi * QKV:(hi + 1) * QKV, :] = wqp[hi, 0:QKV, :]

    def dwq_copy():
        return rc(dwq.at[1], dwq_r, wq_ss.at[1], wq_rs.at[1], mate)

    def dh_pair_copy(kb):
        return rc(dh_send.at[kb], dh_pair.at[kb // 2], dhp_ss.at[kb // 2], dhp_rs.at[kb // 2], PT)

    def dh_copy(kb):
        return rc(dh_send.at[kb], dh_all.at[chip], dh_ss.at[kb // 2], dh_rs.at[chip], kb)

    def dh_finish(kb):
        @pl.when(core == kb % 2)
        def _():
            dh_pair_copy(kb).wait_recv()
            total = (dh_send[kb].astype(F32) + dh_pair[kb // 2].astype(F32)).astype(BF16)
            dh_send[kb] = total

            @pl.when(me != kb)
            def _():
                dh_copy(kb).start()

            @pl.when(me == kb)
            def _():
                dh_all[chip] = total
    @pl.loop(0, 2)
    def _(i):
        hi = 1 - i
        base = pl.multiple_of(QKV * hi, HEAD)

        @pl.when(i == 1)
        def _():
            dwq_copy().start()

        for kb in range(n_dev):
            rows = m256(kb)
            late = slice(kb * TOK, n_dev * TOK)
            for qb in range(kb, n_dev):
                cols = m256(qb)
                for c in range(2):
                    part = slice(c * HALF, c * HALF + HALF)
                    keys = slice(kb * TOK + c * HALF, kb * TOK + c * HALF + HALF)
                    p = jnp.exp2(mm(k_s[hi, keys, :], qkvt[hi, 0:HEAD, cols]) * s_fac - lse[hi, :, cols])
                    if qb == kb:
                        p = jnp.where(keep[part], p, 0.0)
                    dp = mm(v_s[hi, keys, :], do_all[hi, :, cols]).astype(BF16).astype(F32)
                    p_b[kb % 2, part, cols] = p.astype(BF16)
                    ds_b[kb % 2, part, cols] = (p * (dp - delta[hi, :, cols])).astype(BF16)
            dv = mm(p_b[kb % 2, :, late], do_s[hi, late, :])
            dk = mm(ds_b[kb % 2, :, late], q_s[hi, late, :]) * attn_scale
            dq = mm(qkvt[hi, HEAD:HALF, rows], ds_b[kb % 2, :, late])
            if kb == 0:
                dqt[...] = dq
            else:
                dqt[:, late] += dq
            dqkvt[pl.ds(base, HEAD), rows] = (dqt[:, rows] * attn_scale).astype(BF16)
            dqkvt[pl.ds(base + HEAD, HALF), rows] = jnp.concatenate([dk, dv], axis=1).T.astype(BF16)

            @pl.when(i == 1)
            def _():
                dh = mm(dqkvt[:, rows], wq_cat[...], 0, 0)
                dh_send[kb] = dh.astype(BF16)

                @pl.when(core != kb % 2)
                def _():
                    dh_pair_copy(kb).start()

                if kb > 0:
                    dh_finish(kb - 1)


        mine = dqkvt[pl.ds(base, QKV), :]
        dwq[hi, 0:QKV, :] = mm(mine, h1[...])
        dwq[hi, QKV:DW_ROWS, 0:QKV] = mm(jnp.ones((SUB, SEQ), BF16), mine, 1, 1)

    dh_finish(n_dev - 1)
    side_copy(2).start()

    acc[...] = jnp.zeros_like(acc)

    @pl.loop(0, n_dev)
    def _(n):
        for r in range(2):
            rows = slice(r * TOK, r * TOK + TOK)
            acc[rows, :] += mm(ga[n, rows, :], wp[n, 0:TOK, :])

    y_out[...] = (x1[...].astype(F32) + acc[...] + vector(bd)).astype(BF16)

    for t in range(chips):
        @pl.when(chip != t)
        def _():
            rc(dh_send.at[0], dh_all.at[t], dh_ss.at[0], dh_rs.at[t], PT).wait_recv()
    for r in range(FOUR):
        rows = slice(r * HALF, r * HALF + HALF)
        half = slice((r % 2) * HALF, (r % 2) * HALF + HALF)
        first = (r // 2) * (chips // 2)
        dh1 = (dh_all[first, half, :].astype(F32) + dh_all[first + 1, half, :].astype(F32)).astype(BF16).astype(F32)
        x_hat, inv_std = norm_stats(x[rows, :].astype(F32))
        dx_out[rows, :] = (dx1[rows, :].astype(F32) + norm_back(dh1, x_hat, inv_std, gain1)).astype(BF16)
        vec[0:1, :] += jnp.sum(dh1 * x_hat, axis=0, keepdims=True)
        vec[1:2, :] += jnp.sum(dh1, axis=0, keepdims=True)

    def vec_copy(j):
        return rc(vec, vec_all.at[me], v_ss.at[j], v_rs.at[me], j)
    for j in range(n_dev):
        @pl.when(me != j)
        def _():
            vec_copy(j).start()
    vec_all[me] = vec[...]
    for step in range(THREE):
        side_copy(step).wait_recv()
    dwd_out[...] = dwp[THREE, 0:TOK, :] + frx[0:TOK, :]
    dwu_out[...] = (dwp[THREE, TOK:WIDTH, :] + frx[TOK:WIDTH, :]).T
    dbu_out[...] = dwp[THREE, WIDTH:520, 0:TOK] + frx[WIDTH:520, 0:TOK]
    dwo_rx[chip] = dwop[me]
    for t in range(chips):
        @pl.when(chip != t)
        def _():
            rc(dwop.at[0], dwo_rx.at[t], ox_ss.at[0], ox_rs.at[t], PT).wait_recv()
    dwo_out[...] = dwo_rx[0] + dwo_rx[1] + dwo_rx[2] + dwo_rx[THREE]

    dwq_copy().wait_recv()
    dwqkv_out[...] = dwq[0] + dwq_r[...]
    for j in range(n_dev):
        @pl.when(me != j)
        def _():
            rc(vec, vec_all.at[j], v_ss.at[0], v_rs.at[j], PT).wait_recv()
    total = vec_all[0]
    for j in range(1, n_dev):
        total = total + vec_all[j]
    vec_out[...] = total

    wq_copy().wait_send()
    dwq_copy().wait_send()
    for t in range(chips):
        h1_pair(t, False).wait_send()

        @pl.when(chip != t)
        def _():
            wo_copy(t).wait_send()

        wo_pair_copy(t).wait_send()
    for step in range(9):
        w_copy(step).wait_send()
    for step in range(7):
        wo_all_copy(step).wait_send()
    for step in range(THREE):
        h1_copy(step).wait_send()
    for step in range(THREE):
        mate_copy(step).wait_send()
    for which in range(2):
        pair_copy(which).wait_send()
    for step in range(THREE):
        side_copy(step).wait_send()
    for j in range(n_dev):
        @pl.when(me != j)
        def _():
            vec_copy(j).wait_send()
            for hi in range(2):
                o_copy(hi, j).wait_send()

        for st in range(2):
            @pl.when(me != handler(j, st))
            def _():
                do_copy(j, st).wait_send()

        @pl.when(core != j % 2)
        def _():
            dh_pair_copy(j).wait_send()

        @pl.when((core == j % 2) & (me != j))
        def _():
            dh_copy(j).wait_send()


def finish_kernel(y, dx, vec, dwqkv, dwo, dwu, dbu, dwd, y_o, dx_o, v0, v1, dwqkv_o, dbqkv_o, dwo_o, v2, v3, v4, dwu_o, dbu_o, dwd_o, v5):
    y_o[...] = y[...]
    dx_o[...] = dx[...]
    for i, ref in enumerate((v0, v1, v2, v3, v4, v5)):
        ref[...] = vec[i:i + 1, :].reshape(ref.shape)
    dwqkv_o[...] = dwqkv[0:QKV, :]
    for c in range(THREE):
        dbqkv_o[c] = dwqkv[QKV:193, c * HEAD:(c + 1) * HEAD]
    dwo_o[...] = dwo[...]
    dwu_o[...] = dwu[...]
    dbu_o[...] = dbu[0:1, :].reshape(dbu_o.shape)
    dwd_o[...] = dwd[...]


def solution(mesh):
    n_dev = mesh.shape["tp"]

    def device_step(hidden, grad_out, ln1_gain, ln1_bias, w_qkv, b_qkv, w_out, b_out, ln2_gain, ln2_bias, w_up, b_up, w_down, b_down):
        batch, tokens, d = hidden.shape
        rows = batch * tokens
        head = w_qkv.shape[-1]
        seq = tokens * n_dev
        ff = w_up.shape[1]
        chips = n_dev // 2
        attn_scale = head ** -0.5
        sds = jax.ShapeDtypeStruct
        vm = pltpu.VMEM

        def dma(*shape):
            return pltpu.SemaphoreType.DMA(shape)

        vspec = pl.BlockSpec(memory_space=pltpu.VMEM)
        outs = pl.pallas_call(
            lambda *refs: layer_kernel(n_dev, attn_scale, *refs),
            out_shape=(sds((rows, d), BF16), sds((rows, d), BF16), sds((SUB, d), F32), sds((DW_ROWS, d), F32),
                       sds((head, d), F32), sds((d, ff), F32), sds((SUB, ff), F32), sds((ff, d), F32)),
            in_specs=[vspec] * 14,
            out_specs=tuple([vspec] * SUB),
            scratch_shapes=[
                vm((2, tokens, d), BF16), vm((seq, d), BF16), vm((n_dev, WO_ROWS, d), BF16), vm((n_dev, 2 * ff, d), BF16),
                vm((2, WQ_ROWS, d), BF16), vm((d, WIDTH), BF16),
                vm((2, seq, head), BF16), vm((2, seq, head), BF16), vm((2, seq, head), BF16), vm((2, THREE * head, seq), BF16),
                vm((PACK, TOK, TOK), F32), vm((2, 1, seq), F32), vm((2, head, seq), BF16), vm((n_dev * head, rows), BF16),
                vm((n_dev * head, d), BF16), vm((rows, d), BF16), vm((2 * rows, d), BF16), vm((2 * rows, d), BF16),
                vm((n_dev, 2 * rows, ff), BF16), vm((n_dev, 2 * rows, ff), BF16), vm((rows, d), F32), vm((rows, d), BF16),
                vm((n_dev * head, rows), BF16), vm((2, head, seq), BF16), vm((2, seq, head), BF16),
                vm((2, 1, seq), F32), vm((head, seq), F32), vm((2, TOK, seq), BF16), vm((2, TOK, seq), BF16), vm((2, seq, TOK), BF16), vm((6 * head, seq), BF16), vm((6 * head, d), BF16),
                vm((n_dev, tokens, d), BF16), vm((chips, tokens, d), BF16), vm((chips, tokens, d), BF16),
                vm((2, DW_ROWS, d), F32), vm((DW_ROWS, d), F32),
                vm((FOUR, G_ROWS, d), F32), vm((2, G_ROWS, d), F32), vm((G_ROWS, d), F32),
                vm((n_dev, head, d), F32), vm((chips, head, d), F32), vm((chips, head, d), F32),
                vm((SUB, d), F32), vm((n_dev, SUB, d), F32),
                dma(chips), dma(chips), dma(chips), dma(chips), dma(2), dma(2), dma(7), dma(7), dma(2, n_dev), dma(2, n_dev),
                dma(n_dev, 2), dma(2, n_dev), dma(chips), dma(chips), dma(chips), dma(chips),
                dma(9), dma(9), dma(THREE), dma(THREE), dma(2), dma(2), dma(THREE), dma(THREE), dma(chips), dma(chips), dma(chips), dma(chips), dma(n_dev), dma(n_dev),
            ],
            compiler_params=pltpu.CompilerParams(collective_id=0, has_side_effects=True, vmem_limit_bytes=67043328),
            name="layer",
        )(hidden.reshape(rows, d), grad_out.reshape(rows, d), ln1_gain, ln1_bias, b_out, ln2_gain, ln2_bias, b_down,
          w_qkv.transpose(1, 2, THREE, 0).reshape(THREE * head, d), b_qkv, w_out.reshape(head, d), w_up, b_up, w_down)
        v1d = sds((d,), F32)
        y, dx, v0, v1, dwqkv_t, dbqkv, dwo, v2, v3, v4, dwu, dbu, dwd, v5 = pl.pallas_call(
            finish_kernel,
            out_shape=(sds((rows, d), BF16), sds((rows, d), BF16), v1d, v1d, sds((THREE * head, d), F32), sds((THREE, 1, head), F32),
                       sds((head, d), F32), v1d, v1d, v1d, sds((d, ff), F32), sds((ff,), F32), sds((ff, d), F32), v1d),
            in_specs=[vspec] * SUB,
            out_specs=tuple([vspec] * 14),
            name="finish",
        )(*outs)
        return (y.reshape(hidden.shape), dx.reshape(hidden.shape), v0, v1, dwqkv_t.reshape(THREE, 1, head, d).transpose(THREE, 0, 1, 2),
                dbqkv, dwo.reshape(w_out.shape), v2, v3, v4, dwu, dbu, dwd, v5)

    act_spec = P("dp", "tp", None)
    vec_spec = P(None)
    group_vec = P("dp")
    in_specs = (act_spec, act_spec, vec_spec, vec_spec, P(None, None, "tp", None), P(None, "tp", None), P("tp", None, None), vec_spec, vec_spec, vec_spec, P(None, "tp"), P("tp"), P("tp", None), vec_spec)
    out_specs = (act_spec, act_spec, group_vec, group_vec, P("dp", None, "tp", None), P("dp", "tp", None), P(("dp", "tp"), None, None), group_vec, group_vec, group_vec, P("dp", "tp"), P(("dp", "tp")), P(("dp", "tp"), None), group_vec)
    return jax.shard_map(device_step, mesh=mesh, in_specs=in_specs, out_specs=out_specs, check_vma=False)
```
